32 devices in a mesh: groups: 2 (over x), tm: 16 (over z, y, core).
Axes of the slice: x: 2, y: 2, z: 4, core: 2. Of those that a mesh axis runs over, the one named last changes fastest.
Arguments:
- queries: bfloat16 [6144, 2560], P(('groups', 'tm')), parts along dimension 0, may hold values from -6 to 6
- keys: bfloat16 [6144, 2560], P(('groups', 'tm')), parts along dimension 0, may hold values from -6 to 6
- values: bfloat16 [6144, 2560], P(('groups', 'tm')), parts along dimension 0, may hold values from -6 to 6
- q_gain: float32 [2560], replicated, may hold values from 0.5 to 1.5
- k_gain: float32 [2560], replicated, may hold values from 0.5 to 1.5
- out_weight: bfloat16 [2560, 5120], P('tm'), may hold values from -0.125 to 0.125
- out_gate: float32 [5120], replicated, may hold values from 0.5 to 2
- reach: int32 [32, 2], P(('groups', 'tm')), parts along dimension 0, may hold values from 0 to 1
Outputs:
- mixed: bfloat16 [6144, 5120], P(('groups', 'tm')), parts along dimension 0
The draws below stay inside these ranges and needn't reach their ends.
There are 2 independent parts, one for each index of `groups`. The reference program is written for one: setup_inputs(seed, part) draws one part's arguments, and reference() takes and returns one part's arrays. A program takes and returns all parts, laid end to end along the dimension named above; an argument that names none is the same for every part. Nothing has to cross between parts.
Inputs may be any that keep to these rules, and one draw needn't show every extreme that they name: `reach`: requests past the first or last tile are ignored.
All inputs are finite; a program needn't handle non-finite values.
Results may differ from the reference program's by a relative error of at most 0.0076.
Values may be sent and summed in bfloat16 or wider, within the bound.
No kernel may reach another device: no remote copies, remote signals or barrier semaphores. Data moves between devices by JAX's collectives and lax.ppermute only.
A program may use at most 128 MiB of HBM per device.

```python
import math
import jax
import jax.numpy as jnp
from jax import lax

D = 5120
HEADS = 20
HD = 128
TT = 4
TH = 6
TW = 8
TILES = 16
TOKENS = 3072
CHANNELS = 2560


def draw_queries(key, part):
    base = jnp.clip(jax.random.normal(jax.random.fold_in(key, 711), (TOKENS, HEADS * HD), jnp.float32), -6.0, 6.0)
    return base.astype(jnp.bfloat16)


def draw_keys(key, part):
    base = jnp.clip(jax.random.normal(jax.random.fold_in(key, 712), (TOKENS, HEADS * HD), jnp.float32), -6.0, 6.0)
    return base.astype(jnp.bfloat16)


def place_ends(drawn, own_key, least, top_value):
    longest = drawn.shape.index(max(drawn.shape))
    spots = []
    for shift in (0, 1):
        where = [jax.random.randint(jax.random.fold_in(own_key, axis), (), 0, length) for axis, length in enumerate(drawn.shape)]
        where[longest] = (where[longest] + shift) % drawn.shape[longest]
        spots.append(tuple(where))
    return drawn.at[spots[0]].set(least).at[spots[1]].set(top_value)


def block_levels(key, shape, cuts, low, largest):
    level, own = 1.0, jax.random.fold_in(key, 6)
    for axis_at, shards_of in cuts:
        draws = jnp.exp(jax.random.uniform(jax.random.fold_in(own, axis_at), (shards_of,), jnp.float32, low / len(cuts), largest / len(cuts)))
        level = level * jnp.repeat(draws, shape[axis_at] // shards_of).reshape([-1 if axis == axis_at else 1 for axis in range(len(shape))])
    return level


def normal_values(key, shape, scale, most, shards=(), kind=jnp.bfloat16):
    values = jax.random.normal(key, shape, jnp.float32) * scale
    if len(shards) > 0:
        values = block_levels(key, shape, shards, -0.22, 0.18) * values
    return jnp.clip(values, min=-most, max=most).astype(kind)


def setup_inputs(seed: int = 0, part: int = 0) -> dict:
    arg_keys = jax.random.split(jax.random.key(seed), 9)
    own_keys = jax.random.split(jax.random.fold_in(arg_keys[8], part), 9)
    queries = draw_queries(jax.random.fold_in(jax.random.fold_in(arg_keys[8], part), 71), part)
    keys = draw_keys(jax.random.fold_in(jax.random.fold_in(arg_keys[8], part), 71), part)
    values = normal_values(own_keys[2], (TOKENS, CHANNELS), 1.0, 6.0, ((0, 16),))
    q_gain = jnp.clip(1.0 + 0.1 * jax.random.normal(arg_keys[3], (CHANNELS,), jnp.float32), 0.5, 1.5)
    k_gain = jnp.clip(1.0 + 0.1 * jax.random.normal(arg_keys[4], (CHANNELS,), jnp.float32), 0.5, 1.5)
    out_weight = normal_values(arg_keys[5], (CHANNELS, D), CHANNELS ** -0.5, 0.125, ((0, 16),))
    out_gate = jnp.clip(jnp.exp(jax.random.uniform(arg_keys[6], (D,), jnp.float32, math.log(0.5), math.log(2.0))), 0.5, 2.0)
    reach = place_ends(jax.random.randint(own_keys[7], (TILES, 2), 0, 2), jax.random.fold_in(own_keys[7], 1), 0, 1).astype(jnp.int32)
    return dict(queries=queries, keys=keys, values=values, q_gain=q_gain, k_gain=k_gain, out_weight=out_weight, out_gate=out_gate, reach=reach)


def rms_scaled(block, gain):
    values32 = block.astype(jnp.float32)
    inverse = lax.rsqrt(lax.optimization_barrier(jnp.mean(values32 * values32, axis=-1, keepdims=True)) + 1e-06)
    return (values32 * inverse * gain).astype(jnp.bfloat16)

def reference(queries, keys, values, q_gain, k_gain, out_weight, out_gate, reach):
    tile = TT * TH * TW
    scale = HD ** (-0.5)
    q_norm = rms_scaled(queries, q_gain).reshape(TILES, tile, HEADS, HD)
    k_norm = rms_scaled(keys, k_gain).reshape(TILES, tile, HEADS, HD)
    v_tiles = values.reshape(TILES, tile, HEADS, HD)
    padding = jnp.zeros((1, tile, HEADS, HD), jnp.bfloat16)
    key_tiles = jnp.concatenate([padding, k_norm, padding], axis=0)
    val_tiles = jnp.concatenate([padding, v_tiles, padding], axis=0)
    tile_index = jnp.arange(TILES, dtype=jnp.int32)
    valid = jnp.stack([(reach[:, 0] == 1) & (tile_index > 0), tile_index >= 0, (reach[:, 1] == 1) & (tile_index < TILES - 1)], axis=1)

    def one_tile(index):
        index = index.astype(jnp.int32)
        query = q_norm[index].astype(jnp.float32)
        seen_k = lax.dynamic_slice_in_dim(key_tiles, index, 3, 0).reshape(3 * tile, HEADS, HD).astype(jnp.float32)
        seen_v = lax.dynamic_slice_in_dim(val_tiles, index, 3, 0).reshape(3 * tile, HEADS, HD).astype(jnp.float32)
        logits = jnp.einsum('qhd,khd->hqk', query, seen_k) * scale
        mask = jnp.repeat(valid[index], tile)
        logits = jnp.where(mask[None, None, :], logits, -1e+30)
        top = lax.optimization_barrier(jnp.max(logits, axis=-1, keepdims=True))
        expo = jnp.exp(logits - top)
        weights = (expo / lax.optimization_barrier(jnp.sum(expo, axis=-1, keepdims=True))).astype(jnp.bfloat16)
        attended = jnp.einsum('hqk,khd->qhd', weights.astype(jnp.float32), seen_v).astype(jnp.bfloat16)
        attended = attended.reshape(tile, HEADS * HD)
        projected = jnp.dot(attended, out_weight, preferred_element_type=jnp.float32)
        return (out_gate * projected).astype(jnp.bfloat16)
    mixed = lax.map(one_tile, tile_index)
    return mixed.reshape(TOKENS, D)
```

```python
import functools

import jax
import jax.numpy as jnp
from jax import lax
from jax.experimental import pallas as pl
from jax.experimental.pallas import tpu as pltpu
from jax.sharding import PartitionSpec as P

HD = 128


def inverse_rms(ref):
    block = ref[...].astype(jnp.float32)
    return lax.rsqrt(jnp.mean(block * block, axis=-1, keepdims=True) + 1e-06)


def attend_kernel(seen_ref, q_ref, kb_ref, k_ref, ka_ref, vb_ref, v_ref, va_ref, qg_ref, kg_ref, o_ref):
    rows, chans = q_ref.shape
    heads = chans // HD
    scale = HD ** (-0.5)
    bias = [(1.0 - seen_ref[i].astype(jnp.float32)) * -1e30 for i in range(2)]
    q_inv = inverse_rms(q_ref)
    k_inv = [inverse_rms(ref) for ref in (kb_ref, k_ref, ka_ref)]

    def scaled(ref, inv, gain_ref, at):
        block = ref[:, at].astype(jnp.float32)
        return (block * inv * gain_ref[:, at]).astype(jnp.bfloat16)

    def head(h, carry):
        at = pl.ds(pl.multiple_of(h * HD, HD), HD)
        query = scaled(q_ref, q_inv, qg_ref, at)
        parts = []
        for ref, inv, extra in zip((kb_ref, k_ref, ka_ref), k_inv, (bias[0], None, bias[1])):
            key = scaled(ref, inv, kg_ref, at)
            part = lax.dot_general(query, key, (((1,), (1,)), ((), ())), preferred_element_type=jnp.float32) * scale
            parts.append(part if extra is None else part + extra)
        top = functools.reduce(jnp.maximum, [jnp.max(part, axis=-1, keepdims=True) for part in parts])
        expo = [jnp.exp(part - top) for part in parts]
        total = functools.reduce(jnp.add, [jnp.sum(part, axis=-1, keepdims=True) for part in expo])
        share = 1.0 / total
        out = None
        for part, ref in zip(expo, (vb_ref, v_ref, va_ref)):
            weights = (part * share).astype(jnp.bfloat16)
            term = jnp.dot(weights, ref[:, at], preferred_element_type=jnp.float32)
            out = term if out is None else out + term
        o_ref[:, at] = out.astype(jnp.bfloat16)
        return carry

    lax.fori_loop(0, heads, head, 0)


def attend(seen, queries, kb, keys, ka, vb, values, va, q_gain, k_gain):
    rows, chans = queries.shape
    vmem = pl.BlockSpec(memory_space=pltpu.VMEM)
    return pl.pallas_call(
        attend_kernel,
        out_shape=jax.ShapeDtypeStruct((rows, chans), jnp.bfloat16),
        in_specs=[pl.BlockSpec(memory_space=pltpu.SMEM)] + [vmem] * 9,
        out_specs=vmem,
        name="attend",
    )(seen, queries, kb, keys, ka, vb, values, va, q_gain.reshape(1, chans), k_gain.reshape(1, chans))


def local(queries, keys, values, q_gain, k_gain, out_weight, out_gate, reach):
    peers = lax.axis_size("tm")
    groups = lax.axis_size("groups")
    place = lax.axis_index("tm")
    group = lax.axis_index("groups")
    core = place % 2
    side = (place // 2) % 2
    lines = peers // 4
    depth, width = out_weight.shape
    rows, chans = queries.shape
    part = width // (2 * groups)
    first = part * 3 // 5 // 128 * 128

    def core_swap(x):
        return lax.ppermute(x, "tm", [(i, i ^ 1) for i in range(peers)])

    def side_swap(x):
        return lax.ppermute(x, "tm", [(i, i ^ 2) for i in range(peers)])

    def group_swap(x):
        return lax.ppermute(x, "groups", [(i, i ^ 1) for i in range(groups)])

    def diag_swap(x):
        pairs = [(i * peers + j, (i ^ 1) * peers + (j ^ 1)) for i in range(groups) for j in range(peers)]
        return lax.ppermute(x, ("groups", "tm"), pairs)

    def line_gather(x):
        members = [[z * 4 + low for z in range(lines)] for low in range(4)]
        return lax.all_gather(x, "tm", axis_index_groups=members, axis=0)

    def shifted(x, by):
        return lax.ppermute(x, "tm", [(i, i + by) for i in range(peers) if 0 <= i + by < peers])

    mine = lax.dynamic_slice_in_dim(out_weight, (group * 2 + core) * part, part, 1)
    theirs = lax.dynamic_slice_in_dim(out_weight, (group * 2 + 1 - core) * part, part, 1)
    other = core_swap(theirs)
    block = jnp.concatenate([jnp.where(core == 0, mine, other), jnp.where(core == 0, other, mine)], axis=0)
    near, far = block[:, :first], block[:, first:]

    far_other = side_swap(far)
    far_pair = jnp.concatenate([jnp.where(side == 0, far, far_other), jnp.where(side == 0, far_other, far)], axis=0)

    kb, vb = shifted(keys, 1), shifted(values, 1)
    ka, va = shifted(keys, -1), shifted(values, -1)

    near_line = line_gather(near)
    far_all = line_gather(far_pair).reshape(chans, part - first)
    near_other = side_swap(near_line)
    near_all = jnp.stack(
        [jnp.where(side == 0, near_line, near_other), jnp.where(side == 0, near_other, near_line)], axis=1
    ).reshape(chans, first)

    seen = jnp.stack([(reach[0, 0] == 1) & (place > 0), (reach[0, 1] == 1) & (place < peers - 1)]).astype(jnp.int32)
    attended = attend(seen, queries, kb, keys, ka, vb, values, va, q_gain, k_gain)
    att_group = group_swap(attended)
    att_core = core_swap(attended)
    att_diag = core_swap(att_group)
    att = jnp.concatenate([attended, att_core, att_group, att_diag], axis=0)

    gate = lax.dynamic_slice_in_dim(out_gate, (group * 2 + core) * part, part, 0)

    def project(weight, gates):
        out = (gates * jnp.dot(att, weight, preferred_element_type=jnp.float32)).astype(jnp.bfloat16)
        out = out.reshape(4, rows, -1)
        return out[0], core_swap(out[1]), group_swap(out[2]), diag_swap(out[3])

    near_outs = project(near_all, gate[:first])
    far_outs = project(far_all, gate[first:])
    outs = [jnp.concatenate([a, b], axis=1) for a, b in zip(near_outs, far_outs)]

    def ordered(flag, a, b):
        return [jnp.where(flag == 0, a, b), jnp.where(flag == 0, b, a)]

    here = ordered(core, outs[0], outs[1])
    there = ordered(core, outs[2], outs[3])
    pairs = [ordered(group, a, b) for a, b in zip(here, there)]
    return jnp.concatenate([pairs[0][0], pairs[1][0], pairs[0][1], pairs[1][1]], axis=1)


def solution(mesh):
    return jax.shard_map(
        local,
        mesh=mesh,
        in_specs=(
            P(("groups", "tm"), None),
            P(("groups", "tm"), None),
            P(("groups", "tm"), None),
            P(),
            P(),
            P("tm", None),
            P(),
            P(("groups", "tm"), None),
        ),
        out_specs=P(("groups", "tm"), None),
        check_vma=False,
    )
```

```python
import functools

import jax
import jax.numpy as jnp
from jax import lax
from jax.experimental import pallas as pl
from jax.experimental.pallas import tpu as pltpu
from jax.sharding import PartitionSpec as P


HD = 128


def whole(count):
    return [pl.BlockSpec(memory_space=pltpu.VMEM)] * count


def prepare_kernel(q_ref, k_ref, v_ref, qg_ref, kg_ref, qn_ref, *kv_refs):
    def scaled(ref, gain_ref):
        block = ref[...].astype(jnp.float32)
        inverse = lax.rsqrt(jnp.mean(block * block, axis=-1, keepdims=True) + 1e-06)
        return (block * inverse * gain_ref[...]).astype(jnp.bfloat16)

    wide = kv_refs[0].shape[1] // 2
    kn = scaled(k_ref, kg_ref)
    for i, kv_ref in enumerate(kv_refs):
        kv_ref[:, :wide] = kn[:, i * wide : (i + 1) * wide]
        kv_ref[:, wide:] = v_ref[:, i * wide : (i + 1) * wide]
    qn_ref[...] = scaled(q_ref, qg_ref)


def prepare(queries, keys, values, q_gain, k_gain, chunks):
    rows, chans = queries.shape
    kv = jax.ShapeDtypeStruct((rows, 2 * chans // chunks), jnp.bfloat16)
    return pl.pallas_call(
        prepare_kernel,
        out_shape=[jax.ShapeDtypeStruct((rows, chans), jnp.bfloat16)] + [kv] * chunks,
        in_specs=whole(5),
        out_specs=whole(1 + chunks),
        name="prepare",
    )(queries, keys, values, q_gain.reshape(1, chans), k_gain.reshape(1, chans))


def attend_kernel(seen_ref, q_ref, kb_ref, k_ref, ka_ref, vb_ref, v_ref, va_ref, o_ref):
    scale = HD ** (-0.5)
    bias = [(1.0 - seen_ref[i].astype(jnp.float32)) * -1e30 for i in range(2)]
    for h in range(q_ref.shape[1] // HD):
        at = slice(h * HD, (h + 1) * HD)
        query = q_ref[:, at]
        parts = []
        for ref, extra in ((kb_ref, bias[0]), (k_ref, None), (ka_ref, bias[1])):
            part = lax.dot_general(query, ref[:, at], (((1,), (1,)), ((), ())), preferred_element_type=jnp.float32)
            part = part * scale
            parts.append(part if extra is None else part + extra)
        top = functools.reduce(jnp.maximum, [jnp.max(part, axis=-1, keepdims=True) for part in parts])
        expo = [jnp.exp(part - top) for part in parts]
        total = functools.reduce(jnp.add, [jnp.sum(part, axis=-1, keepdims=True) for part in expo])
        share = 1.0 / total
        out = None
        for part, ref in zip(expo, (vb_ref, v_ref, va_ref)):
            weights = (part * share).astype(jnp.bfloat16)
            term = jnp.dot(weights, ref[:, at], preferred_element_type=jnp.float32)
            out = term if out is None else out + term
        o_ref[:, at] = out.astype(jnp.bfloat16)


def attend(seen, qn, before, kv, after, chunk, chunks):
    rows, chans = qn.shape
    wide = chans // chunks
    heads = wide // HD
    step = next(n for n in (5, 4, 3, 2, 1) if heads % n == 0)
    cols = step * HD
    steps = wide // cols
    q_spec = pl.BlockSpec((rows, cols), lambda i: (0, chunk * steps + i))
    k_spec = pl.BlockSpec((rows, cols), lambda i: (0, i))
    v_spec = pl.BlockSpec((rows, cols), lambda i: (0, steps + i))
    return pl.pallas_call(
        attend_kernel,
        grid=(steps,),
        out_shape=jax.ShapeDtypeStruct((rows, wide), jnp.bfloat16),
        in_specs=[pl.BlockSpec(memory_space=pltpu.SMEM), q_spec] + [k_spec] * 3 + [v_spec] * 3,
        out_specs=pl.BlockSpec((rows, cols), lambda i: (0, i)),
    )(seen, qn, before, kv, after, before, kv, after)


def project_kernel(count, starts_ref, gate_ref, *refs):
    slots = starts_ref.shape[0]
    att_refs, w_refs = refs[:count], refs[count : count + slots]
    outs = refs[count + slots : count + slots + 4]
    a_ref, w_ref, sems = refs[count + slots + 4 :]
    rows, wide = att_refs[0].shape
    depth = w_refs[0].shape[0]
    chunks = count // 4
    copies = []
    for i, ref in enumerate(w_refs):
        start = pl.multiple_of(starts_ref[i], depth)
        copies.append(pltpu.make_async_copy(ref, w_ref.at[pl.ds(start, depth)], sems.at[i]))
    for i, ref in enumerate(att_refs):
        p, j = i // chunks, i % chunks
        dst = a_ref.at[pl.ds(p * rows, rows), pl.ds(j * wide, wide)]
        copies.append(pltpu.make_async_copy(ref, dst, sems.at[slots + i]))
    for copy in copies:
        copy.start()
    for copy in copies:
        copy.wait()
    for p in range(4):
        acc = jnp.dot(a_ref[p * rows : (p + 1) * rows, :], w_ref[...], preferred_element_type=jnp.float32)
        outs[p][...] = (gate_ref[...] * acc).astype(jnp.bfloat16)


def project(starts, gate, att, weights):
    rows, wide = att[0].shape
    chans = wide * len(att) // 4
    cols = weights[0].shape[1]
    slots = len(weights)
    anywhere = pl.BlockSpec(memory_space=pl.ANY)
    return pl.pallas_call(
        functools.partial(project_kernel, len(att)),
        out_shape=[jax.ShapeDtypeStruct((rows, cols), jnp.bfloat16)] * 4,
        in_specs=[pl.BlockSpec(memory_space=pltpu.SMEM)] + whole(1) + [anywhere] * (len(att) + slots),
        out_specs=whole(4),
        scratch_shapes=[
            pltpu.VMEM((4 * rows, chans), jnp.bfloat16),
            pltpu.VMEM((chans, cols), jnp.bfloat16),
            pltpu.SemaphoreType.DMA((slots + len(att),)),
        ],
    )(starts, gate.reshape(1, cols), *att, *weights)


def place_kernel(starts_ref, *refs):
    pieces, out_ref, sems = refs[:-2], refs[-2], refs[-1]
    cols = pieces[0].shape[1]
    copies = []
    for i, ref in enumerate(pieces):
        start = pl.multiple_of(starts_ref[i], 128)
        copies.append(pltpu.make_async_copy(ref, out_ref.at[:, pl.ds(start, cols)], sems.at[i]))
    for copy in copies:
        copy.start()
    for copy in copies:
        copy.wait()


def place_pieces(starts, pieces):
    rows, cols = pieces[0].shape
    anywhere = pl.BlockSpec(memory_space=pl.ANY)
    return pl.pallas_call(
        place_kernel,
        out_shape=jax.ShapeDtypeStruct((rows, cols * len(pieces)), jnp.bfloat16),
        in_specs=[pl.BlockSpec(memory_space=pltpu.SMEM)] + [anywhere] * len(pieces),
        out_specs=anywhere,
        scratch_shapes=[pltpu.SemaphoreType.DMA((len(pieces),))],
        name="place",
    )(starts, *pieces)


def local(queries, keys, values, q_gain, k_gain, out_weight, out_gate, reach):
    peers = lax.axis_size("tm")
    place = lax.axis_index("tm")
    group = lax.axis_index("groups")
    low = place % 4
    line = place // 4
    lines = peers // 4
    depth, width = out_weight.shape
    _, chans = queries.shape
    cols = width // 8
    chunks = 2 if chans // HD % 2 == 0 else 1

    def swap(x, bits):
        return lax.ppermute(x, "tm", [(i, i ^ bits) for i in range(peers)])

    def group_swap(x):
        return lax.ppermute(x, "groups", [(0, 1), (1, 0)])

    def along(x, moves):
        return lax.ppermute(x, "tm", [(4 * a + i, 4 * b + i) for a, b in moves for i in range(4)])

    def shifted(x, by):
        return lax.ppermute(x, "tm", [(i, i + by) for i in range(peers) if 0 <= i + by < peers])

    def choose(flag, a, b):
        return jnp.where(flag, a, b)

    def column(quarter, share):
        return (quarter * 2 + share) * cols

    def weight_part(quarter):
        return lax.dynamic_slice_in_dim(out_weight, column(quarter, group), cols, 1)

    parts = [weight_part(low)] + [swap(weight_part(low ^ i), i) for i in (1, 2, 3)]
    odd, upper = (low % 2) == 1, low >= 2
    pairs = [
        jnp.concatenate([choose(odd, b, a), choose(odd, a, b)], axis=0)
        for a, b in ((parts[0], parts[1]), (parts[2], parts[3]))
    ]
    block = jnp.concatenate([choose(upper, pairs[1], pairs[0]), choose(upper, pairs[0], pairs[1])], axis=0)

    qn, *kvs = prepare(queries, keys, values, q_gain, k_gain, chunks)
    before = [shifted(kv, 1) for kv in kvs]
    after = [shifted(kv, -1) for kv in kvs]

    if lines == 4:
        middle = (line == 1) | (line == 2)
        near = along(block, ((0, 1), (1, 0), (2, 3), (3, 2)))
        across = along(block, ((1, 2), (2, 1)))
        across_far = along(near, ((1, 2), (2, 1)))
        edge = along(across, ((1, 0), (2, 3)))
        edge_far = along(across_far, ((1, 0), (2, 3)))
        second = choose(middle, across_far, edge)
        third = choose(middle, across, edge_far)
        slots = [block, near, second, third]
        starts = jnp.stack([(line ^ i) * (4 * depth) for i in range(4)]).astype(jnp.int32)
    else:
        members = [[z * 4 + i for z in range(lines)] for i in range(4)]
        slots = [lax.all_gather(block, "tm", axis_index_groups=members, axis=0, tiled=True)]
        starts = jnp.zeros((1,), jnp.int32)
    shares = [slots, [group_swap(slot) for slot in slots]]

    seen = jnp.stack([(reach[0, 0] == 1) & (place > 0), (reach[0, 1] == 1) & (place < peers - 1)]).astype(jnp.int32)
    att = [[None] * chunks for _ in range(4)]
    for i in range(chunks):
        own = attend(seen, qn, before[i], kvs[i], after[i], i, chunks)
        att[0][i] = own
        att[2][i] = swap(own, 2)
        att[1][i] = swap(own, 1)
        att[3][i] = swap(att[2][i], 1)
    att = [piece for pieces in att for piece in pieces]

    outs, columns = [], []
    for j in range(2):
        share = group ^ j
        gate = lax.dynamic_slice_in_dim(out_gate, column(low, share), cols, 0)
        made = project(starts, gate, att, shares[j])
        outs += [made[0]] + [swap(made[i], i) for i in (1, 2, 3)]
        columns += [column(low ^ i, share) for i in range(4)]
    return place_pieces(jnp.stack(columns).astype(jnp.int32), outs)


def solution(mesh):
    return jax.shard_map(
        local,
        mesh=mesh,
        in_specs=(
            P(("groups", "tm"), None),
            P(("groups", "tm"), None),
            P(("groups", "tm"), None),
            P(),
            P(),
            P("tm", None),
            P(),
            P(("groups", "tm"), None),
        ),
        out_specs=P(("groups", "tm"), None),
        check_vma=False,
    )
```

```python
import functools

import jax
import jax.numpy as jnp
from jax import lax
from jax.experimental import pallas as pl
from jax.experimental.pallas import tpu as pltpu
from jax.sharding import PartitionSpec as P


HD = 128


def whole(count):
    return [pl.BlockSpec(memory_space=pltpu.VMEM)] * count


def norm_kernel(x_ref, gain_ref, *out_refs):
    wide = out_refs[0].shape[1]
    block = x_ref[...].astype(jnp.float32)
    inverse = lax.rsqrt(jnp.mean(block * block, axis=-1, keepdims=True) + 1e-06)
    for i in range(x_ref.shape[1] // HD):
        piece = x_ref[:, i * HD : (i + 1) * HD].astype(jnp.float32)
        at = i * HD % wide
        scaled = piece * inverse * gain_ref[i : i + 1, :]
        out_refs[i * HD // wide][:, at : at + HD] = scaled.astype(jnp.bfloat16)


def norm(x, gain, chunks):
    rows, chans = x.shape
    out = jax.ShapeDtypeStruct((rows, chans // chunks), jnp.bfloat16)
    return pl.pallas_call(
        norm_kernel, out_shape=[out] * chunks, in_specs=whole(2), out_specs=whole(chunks)
    )(x, gain.reshape(chans // HD, HD))


def attend_kernel(seen_ref, q_ref, kb_ref, k_ref, ka_ref, vb_ref, v_ref, va_ref, o_ref):
    scale = HD ** (-0.5)
    bias = [(1.0 - seen_ref[i].astype(jnp.float32)) * -1e30 for i in range(2)]
    for h in range(q_ref.shape[1] // HD):
        at = slice(h * HD, (h + 1) * HD)
        query = q_ref[:, at]
        parts = []
        for ref, extra in ((kb_ref, bias[0]), (k_ref, None), (ka_ref, bias[1])):
            part = lax.dot_general(query, ref[:, at], (((1,), (1,)), ((), ())), preferred_element_type=jnp.float32)
            part = part * scale
            parts.append(part if extra is None else part + extra)
        top = functools.reduce(jnp.maximum, [jnp.max(part, axis=-1, keepdims=True) for part in parts])
        expo = [jnp.exp(part - top) for part in parts]
        total = functools.reduce(jnp.add, [jnp.sum(part, axis=-1, keepdims=True) for part in expo])
        share = 1.0 / total
        out = None
        for part, ref in zip(expo, (vb_ref, v_ref, va_ref)):
            weights = (part * share).astype(jnp.bfloat16)
            term = jnp.dot(weights, ref[:, at], preferred_element_type=jnp.float32)
            out = term if out is None else out + term
        o_ref[:, at] = out.astype(jnp.bfloat16)


def attend(seen, qn, keys, values, chunk):
    rows, _ = values[0].shape
    wide = qn.shape[1]
    heads = wide // HD
    step = next(n for n in (5, 4, 3, 2, 1) if heads % n == 0)
    cols = step * HD
    steps = wide // cols
    k_spec = pl.BlockSpec((rows, cols), lambda i: (0, i))
    v_spec = pl.BlockSpec((rows, cols), lambda i: (0, chunk * steps + i))
    return pl.pallas_call(
        attend_kernel,
        grid=(steps,),
        out_shape=jax.ShapeDtypeStruct((rows, wide), jnp.bfloat16),
        in_specs=[pl.BlockSpec(memory_space=pltpu.SMEM)] + [k_spec] * 4 + [v_spec] * 3,
        out_specs=k_spec,
    )(seen, qn, *keys, *values)


def project_kernel(count, starts_ref, gate_ref, *refs):
    slots = starts_ref.shape[0]
    att_refs, w_refs = refs[:count], refs[count : count + slots]
    outs = refs[count + slots : count + slots + 4]
    w_ref, sems = refs[count + slots + 4 :]
    wide = att_refs[0].shape[1]
    depth = w_refs[0].shape[0]
    chunks = count // 4
    copies = []
    for i, ref in enumerate(w_refs):
        start = pl.multiple_of(starts_ref[i], depth)
        copies.append(pltpu.make_async_copy(ref, w_ref.at[pl.ds(start, depth)], sems.at[i]))
    for copy in copies:
        copy.start()
    for copy in copies:
        copy.wait()
    for p in range(4):
        acc = None
        for j in range(chunks):
            term = jnp.dot(
                att_refs[p * chunks + j][...],
                w_ref[j * wide : (j + 1) * wide, :],
                preferred_element_type=jnp.float32,
            )
            acc = term if acc is None else acc + term
        outs[p][...] = (gate_ref[...] * acc).astype(jnp.bfloat16)


def project(starts, gate, att, weights):
    rows, wide = att[0].shape
    chans = wide * len(att) // 4
    cols = weights[0].shape[1]
    slots = len(weights)
    return pl.pallas_call(
        functools.partial(project_kernel, len(att)),
        out_shape=[jax.ShapeDtypeStruct((rows, cols), jnp.bfloat16)] * 4,
        in_specs=[pl.BlockSpec(memory_space=pltpu.SMEM)]
        + whole(1 + len(att))
        + [pl.BlockSpec(memory_space=pl.ANY)] * slots,
        out_specs=whole(4),
        scratch_shapes=[pltpu.VMEM((chans, cols), jnp.bfloat16), pltpu.SemaphoreType.DMA((slots,))],
    )(starts, gate.reshape(1, cols), *att, *weights)


def place_kernel(starts_ref, *refs):
    pieces, out_ref = refs[:-1], refs[-1]
    cols = pieces[0].shape[1]
    for i, ref in enumerate(pieces):
        start = pl.multiple_of(starts_ref[i], 128)
        out_ref[:, pl.ds(start, cols)] = ref[...]


def place_pieces(starts, pieces):
    rows, cols = pieces[0].shape
    return pl.pallas_call(
        place_kernel,
        out_shape=jax.ShapeDtypeStruct((rows, cols * len(pieces)), jnp.bfloat16),
        in_specs=[pl.BlockSpec(memory_space=pltpu.SMEM)] + whole(len(pieces)),
        out_specs=pl.BlockSpec(memory_space=pltpu.VMEM),
        name="place",
    )(starts, *pieces)


def local(queries, keys, values, q_gain, k_gain, out_weight, out_gate, reach):
    peers = lax.axis_size("tm")
    place = lax.axis_index("tm")
    group = lax.axis_index("groups")
    low = place % 4
    line = place // 4
    lines = peers // 4
    depth, width = out_weight.shape
    _, chans = queries.shape
    cols = width // 8
    chunks = 2 if chans // HD % 2 == 0 else 1

    def swap(x, bits):
        return lax.ppermute(x, "tm", [(i, i ^ bits) for i in range(peers)])

    def group_swap(x):
        return lax.ppermute(x, "groups", [(0, 1), (1, 0)])

    def along(x, moves):
        return lax.ppermute(x, "tm", [(4 * a + i, 4 * b + i) for a, b in moves for i in range(4)])

    def shifted(x, by):
        return lax.ppermute(x, "tm", [(i, i + by) for i in range(peers) if 0 <= i + by < peers])

    def choose(flag, a, b):
        return jnp.where(flag, a, b)

    def column(quarter, share):
        return (quarter * 2 + share) * cols

    def weight_part(quarter):
        return lax.dynamic_slice_in_dim(out_weight, column(quarter, group), cols, 1)

    cuts = lax.optimization_barrier([weight_part(low ^ i) for i in range(4)])
    parts = [cuts[0]] + [swap(cuts[i], i) for i in (1, 2, 3)]
    odd, upper = (low % 2) == 1, low >= 2
    pairs = [
        jnp.concatenate([choose(odd, b, a), choose(odd, a, b)], axis=0)
        for a, b in ((parts[0], parts[1]), (parts[2], parts[3]))
    ]
    block = jnp.concatenate([choose(upper, pairs[1], pairs[0]), choose(upper, pairs[0], pairs[1])], axis=0)

    vals = [shifted(values, 1), values, shifted(values, -1)]
    kns = norm(keys, k_gain, chunks)
    keyed = [[shifted(kn, 1), kn, shifted(kn, -1)] for kn in kns]
    qns = norm(queries, q_gain, chunks)

    if lines == 4:
        middle = (line == 1) | (line == 2)
        near = along(block, ((0, 1), (1, 0), (2, 3), (3, 2)))
        across = along(block, ((1, 2), (2, 1)))
        across_far = along(near, ((1, 2), (2, 1)))
        edge = along(across, ((1, 0), (2, 3)))
        edge_far = along(across_far, ((1, 0), (2, 3)))
        second = choose(middle, across_far, edge)
        third = choose(middle, across, edge_far)
        slots = [block, near, second, third]
        starts = jnp.stack([(line ^ i) * (4 * depth) for i in range(4)]).astype(jnp.int32)
    else:
        members = [[z * 4 + i for z in range(lines)] for i in range(4)]
        slots = [lax.all_gather(block, "tm", axis_index_groups=members, axis=0, tiled=True)]
        starts = jnp.zeros((1,), jnp.int32)
    shares = [slots, [group_swap(slot) for slot in slots]]

    seen = jnp.stack([(reach[0, 0] == 1) & (place > 0), (reach[0, 1] == 1) & (place < peers - 1)]).astype(jnp.int32)
    att = [[None] * chunks for _ in range(4)]
    for i in range(chunks):
        own = attend(seen, qns[i], keyed[i], vals, i)
        att[0][i] = own
        att[2][i] = swap(own, 2)
        att[1][i] = swap(own, 1)
        att[3][i] = swap(att[2][i], 1)
    att = [piece for pieces in att for piece in pieces]

    outs, columns = [], []
    for j in range(2):
        share = group ^ j
        gate = lax.dynamic_slice_in_dim(out_gate, column(low, share), cols, 0)
        made = project(starts, gate, att, shares[j])
        outs += [made[0]] + [swap(made[i], i) for i in (1, 2, 3)]
        columns += [column(low ^ i, share) for i in range(4)]
    return place_pieces(jnp.stack(columns).astype(jnp.int32), outs)


def solution(mesh):
    return jax.shard_map(
        local,
        mesh=mesh,
        in_specs=(
            P(("groups", "tm"), None),
            P(("groups", "tm"), None),
            P(("groups", "tm"), None),
            P(),
            P(),
            P("tm", None),
            P(),
            P(("groups", "tm"), None),
        ),
        out_specs=P(("groups", "tm"), None),
        check_vma=False,
    )
```

```python
import functools

import jax
import jax.numpy as jnp
from jax import lax
from jax.experimental import pallas as pl
from jax.experimental.pallas import tpu as pltpu
from jax.sharding import PartitionSpec as P


HD = 128


def whole(count):
    return [pl.BlockSpec(memory_space=pltpu.VMEM)] * count


def scaled_heads(x_ref, gain_ref):
    block = x_ref[...].astype(jnp.float32)
    inverse = lax.rsqrt(jnp.mean(block * block, axis=-1, keepdims=True) + 1e-06)
    for i in range(x_ref.shape[1] // HD):
        piece = x_ref[:, i * HD : (i + 1) * HD].astype(jnp.float32)
        yield i, (piece * inverse * gain_ref[i : i + 1, :]).astype(jnp.bfloat16)


def norm_kernel(x_ref, gain_ref, out_ref):
    for i, piece in scaled_heads(x_ref, gain_ref):
        out_ref[:, i * HD : (i + 1) * HD] = piece


def pair_kernel(k_ref, v_ref, gain_ref, *out_refs):
    wide = out_refs[0].shape[1] // 2
    for i, piece in scaled_heads(k_ref, gain_ref):
        at = i * HD % wide
        out_refs[i * HD // wide][:, at : at + HD] = piece
    for i, ref in enumerate(out_refs):
        ref[:, wide:] = v_ref[:, i * wide : (i + 1) * wide]


def norm(x, gain):
    return pl.pallas_call(
        norm_kernel,
        out_shape=jax.ShapeDtypeStruct(x.shape, jnp.bfloat16),
        in_specs=whole(2),
        out_specs=pl.BlockSpec(memory_space=pltpu.VMEM),
    )(x, gain.reshape(-1, HD))


def pair(keys, values, gain, chunks):
    rows, chans = keys.shape
    out = jax.ShapeDtypeStruct((rows, 2 * chans // chunks), jnp.bfloat16)
    return pl.pallas_call(
        pair_kernel, out_shape=[out] * chunks, in_specs=whole(3), out_specs=whole(chunks)
    )(keys, values, gain.reshape(-1, HD))


def attend_kernel(relayed, reach_ref, q_ref, *refs):
    sources = len(refs) // 2
    o_ref = refs[-1]
    k_refs, v_refs = refs[:sources], refs[sources : 2 * sources]
    scale = HD ** (-0.5)
    place = lax.axis_index("tm")
    peers = lax.axis_size("tm")
    low = place % 4
    seen = ((reach_ref[0, 0] == 1) & (place > 0), (reach_ref[0, 1] == 1) & (place < peers - 1))
    bias = [jnp.where(flag, 0.0, -1e30).astype(jnp.float32) for flag in seen]

    def three(group, at):
        before, own, after = [ref[:, at] for ref in group[:3]]
        if relayed:
            other = group[3][:, at]
            before = jnp.where(low == 0, other, before)
            after = jnp.where(low == 3, other, after)
        return before, own, after

    for h in range(q_ref.shape[1] // HD):
        at = slice(h * HD, (h + 1) * HD)
        query = q_ref[:, at]
        parts = []
        for key, extra in zip(three(k_refs, at), (bias[0], None, bias[1])):
            part = lax.dot_general(query, key, (((1,), (1,)), ((), ())), preferred_element_type=jnp.float32)
            part = part * scale
            parts.append(part if extra is None else part + extra)
        top = functools.reduce(jnp.maximum, [jnp.max(part, axis=-1, keepdims=True) for part in parts])
        expo = [jnp.exp(part - top) for part in parts]
        total = functools.reduce(jnp.add, [jnp.sum(part, axis=-1, keepdims=True) for part in expo])
        share = 1.0 / total
        out = None
        for part, value in zip(expo, three(v_refs, at)):
            weights = (part * share).astype(jnp.bfloat16)
            term = jnp.dot(weights, value, preferred_element_type=jnp.float32)
            out = term if out is None else out + term
        o_ref[:, at] = out.astype(jnp.bfloat16)


def attend(reach, qn, pairs, chunk):
    rows, double = pairs[0].shape
    wide = double // 2
    heads = wide // HD
    step = next(n for n in (5, 4, 3, 2, 1) if heads % n == 0)
    cols = step * HD
    steps = wide // cols
    q_spec = pl.BlockSpec((rows, cols), lambda i: (0, chunk * steps + i))
    k_spec = pl.BlockSpec((rows, cols), lambda i: (0, i))
    v_spec = pl.BlockSpec((rows, cols), lambda i: (0, steps + i))
    return pl.pallas_call(
        functools.partial(attend_kernel, len(pairs) == 4),
        grid=(steps,),
        out_shape=jax.ShapeDtypeStruct((rows, wide), jnp.bfloat16),
        in_specs=[pl.BlockSpec(memory_space=pltpu.SMEM), q_spec] + [k_spec] * len(pairs) + [v_spec] * len(pairs),
        out_specs=k_spec,
    )(reach, qn, *pairs, *pairs)


def project_kernel(count, share, gate_ref, *refs):
    slots = len(refs) - count - 6
    att_refs, w_refs = refs[:count], refs[count : count + slots]
    outs = refs[count + slots : count + slots + 4]
    w_ref, sems = refs[count + slots + 4 :]
    wide = att_refs[0].shape[1]
    depth, cols = w_refs[0].shape
    chunks = count // 4
    place = lax.axis_index("tm")
    line = place // 4
    copies = []
    for i, ref in enumerate(w_refs):
        start = pl.multiple_of((line ^ i) * depth, depth) if slots > 1 else 0
        copies.append(pltpu.make_async_copy(ref, w_ref.at[pl.ds(start, depth)], sems.at[i]))
    for copy in copies:
        copy.start()
    for copy in copies:
        copy.wait()
    first = ((place % 4) * 2 + (lax.axis_index("groups") ^ share)) * (cols // HD)
    for p in range(4):
        acc = None
        for j in range(chunks):
            term = jnp.dot(
                att_refs[p * chunks + j][...],
                w_ref[j * wide : (j + 1) * wide, :],
                preferred_element_type=jnp.float32,
            )
            acc = term if acc is None else acc + term
        for b in range(cols // HD):
            at = slice(b * HD, (b + 1) * HD)
            outs[p][:, at] = (gate_ref[pl.ds(first + b, 1), :] * acc[:, at]).astype(jnp.bfloat16)


def project(gate, att, weights, share):
    rows, wide = att[0].shape
    chans = wide * len(att) // 4
    cols = weights[0].shape[1]
    slots = len(weights)
    return pl.pallas_call(
        functools.partial(project_kernel, len(att), share),
        out_shape=[jax.ShapeDtypeStruct((rows, cols), jnp.bfloat16)] * 4,
        in_specs=whole(1 + len(att)) + [pl.BlockSpec(memory_space=pl.ANY)] * slots,
        out_specs=whole(4),
        scratch_shapes=[pltpu.VMEM((chans, cols), jnp.bfloat16), pltpu.SemaphoreType.DMA((slots,))],
    )(gate.reshape(-1, HD), *att, *weights)


def place_kernel(*refs):
    pieces, out_ref = refs[:-1], refs[-1]
    cols = pieces[0].shape[1]
    low = lax.axis_index("tm") % 4
    group = lax.axis_index("groups")
    for i, ref in enumerate(pieces):
        start = pl.multiple_of(((low ^ (i % 4)) * 2 + (group ^ (i // 4))) * cols, HD)
        out_ref[:, pl.ds(start, cols)] = ref[...]


def place_pieces(pieces):
    rows, cols = pieces[0].shape
    return pl.pallas_call(
        place_kernel,
        out_shape=jax.ShapeDtypeStruct((rows, cols * len(pieces)), jnp.bfloat16),
        in_specs=whole(len(pieces)),
        out_specs=pl.BlockSpec(memory_space=pltpu.VMEM),
        name="place",
    )(*pieces)


def local(queries, keys, values, q_gain, k_gain, out_weight, out_gate, reach):
    peers = lax.axis_size("tm")
    place = lax.axis_index("tm")
    group = lax.axis_index("groups")
    low = place % 4
    line = place // 4
    lines = peers // 4
    _, width = out_weight.shape
    _, chans = queries.shape
    cols = width // 8
    chunks = 2 if chans // HD % 2 == 0 else 1

    def swap(x, bits):
        return lax.ppermute(x, "tm", [(i, i ^ bits) for i in range(peers)])

    def group_swap(x):
        return lax.ppermute(x, "groups", [(0, 1), (1, 0)])

    def along(x, moves):
        return lax.ppermute(x, "tm", [(4 * a + i, 4 * b + i) for a, b in moves for i in range(4)])

    def send(x, pairs):
        return lax.ppermute(x, "tm", pairs)

    up = [(i, i + 1) for i in range(peers - 1)]
    down = [(j, i) for i, j in up]

    def inside(pairs):
        return [(i, j) for i, j in pairs if i // 4 == j // 4]

    def choose(flag, a, b):
        return jnp.where(flag, a, b)

    def column(quarter, share):
        return (quarter * 2 + share) * cols

    def weight_part(quarter):
        return lax.dynamic_slice_in_dim(out_weight, column(quarter, group), cols, 1)

    cuts = lax.optimization_barrier([weight_part(low ^ i) for i in range(4)])
    parts = [cuts[0]] + [swap(cuts[i], i) for i in (1, 2, 3)]
    odd, upper = (low % 2) == 1, low >= 2
    halves = [
        jnp.concatenate([choose(odd, b, a), choose(odd, a, b)], axis=0)
        for a, b in ((parts[0], parts[1]), (parts[2], parts[3]))
    ]
    block = jnp.concatenate([choose(upper, halves[1], halves[0]), choose(upper, halves[0], halves[1])], axis=0)

    pairs = pair(keys, values, k_gain, chunks)
    seen = [[send(kv, up), kv, send(kv, down)] for kv in pairs[:1]]
    for i, kv in enumerate(pairs[1:], 1):
        over = send(kv, [(4 * z + 3, 4 * z + 1) for z in range(lines)] + [(4 * z, 4 * z + 2) for z in range(lines)])
        hops = [(4 * z + 1, 4 * z + 4) for z in range(lines - 1)] + [(4 * z + 2, 4 * z - 1) for z in range(1, lines)]
        over = send(over, hops)
        seen.append([send(kv, inside(up)), kv, send(kv, inside(down)), over])
    qn = norm(queries, q_gain)

    if lines == 4:
        middle = (line == 1) | (line == 2)
        near = along(block, ((0, 1), (1, 0), (2, 3), (3, 2)))
        across = along(block, ((1, 2), (2, 1)))
        across_far = along(near, ((1, 2), (2, 1)))
        edge = along(across, ((1, 0), (2, 3)))
        edge_far = along(across_far, ((1, 0), (2, 3)))
        second = choose(middle, across_far, edge)
        third = choose(middle, across, edge_far)
        slots = [block, near, second, third]
    else:
        members = [[z * 4 + i for z in range(lines)] for i in range(4)]
        slots = [lax.all_gather(block, "tm", axis_index_groups=members, axis=0, tiled=True)]
    shares = [slots, [group_swap(slot) for slot in slots]]

    att = [[None] * chunks for _ in range(4)]
    for i in range(chunks):
        own = attend(reach, qn, seen[i], i)
        att[0][i] = own
        att[2][i] = swap(own, 2)
        att[1][i] = swap(own, 1)
        att[3][i] = swap(att[2][i], 1)
    att = [piece for pieces in att for piece in pieces]

    outs = []
    for j in range(2):
        made = project(out_gate, att, shares[j], j)
        outs += [made[0]] + [swap(made[i], i) for i in (1, 2, 3)]
    return place_pieces(outs)


def solution(mesh):
    return jax.shard_map(
        local,
        mesh=mesh,
        in_specs=(
            P(("groups", "tm"), None),
            P(("groups", "tm"), None),
            P(("groups", "tm"), None),
            P(),
            P(),
            P("tm", None),
            P(),
            P(("groups", "tm"), None),
        ),
        out_specs=P(("groups", "tm"), None),
        check_vma=False,
    )
```

```python
import functools

import jax
import jax.numpy as jnp
from jax import lax
from jax.experimental import pallas as pl
from jax.experimental.pallas import tpu as pltpu
from jax.sharding import PartitionSpec as P


HD = 128


def whole(count):
    return [pl.BlockSpec(memory_space=pltpu.VMEM)] * count


def scaled_heads(x_ref, gain_ref):
    block = x_ref[...].astype(jnp.float32)
    inverse = lax.rsqrt(jnp.mean(block * block, axis=-1, keepdims=True) + 1e-06)
    for i in range(x_ref.shape[1] // HD):
        piece = x_ref[:, i * HD : (i + 1) * HD].astype(jnp.float32)
        yield i, (piece * inverse * gain_ref[i : i + 1, :]).astype(jnp.bfloat16)


def norm_kernel(x_ref, gain_ref, out_ref):
    for i, piece in scaled_heads(x_ref, gain_ref):
        out_ref[:, i * HD : (i + 1) * HD] = piece


def pair_kernel(k_ref, v_ref, gain_ref, out_ref):
    chans = k_ref.shape[1]
    for i, piece in scaled_heads(k_ref, gain_ref):
        out_ref[:, i * HD : (i + 1) * HD] = piece
    out_ref[:, chans:] = v_ref[...]


def norm(x, gain):
    return pl.pallas_call(
        norm_kernel,
        out_shape=jax.ShapeDtypeStruct(x.shape, jnp.bfloat16),
        in_specs=whole(2),
        out_specs=pl.BlockSpec(memory_space=pltpu.VMEM),
    )(x, gain.reshape(-1, HD))


def pair(keys, values, gain):
    rows, chans = keys.shape
    return pl.pallas_call(
        pair_kernel,
        out_shape=jax.ShapeDtypeStruct((rows, 2 * chans), jnp.bfloat16),
        in_specs=whole(3),
        out_specs=pl.BlockSpec(memory_space=pltpu.VMEM),
    )(keys, values, gain.reshape(-1, HD))


def attend_kernel(reach_ref, q_ref, kb_ref, k_ref, ka_ref, vb_ref, v_ref, va_ref, o_ref):
    scale = HD ** (-0.5)
    place = lax.axis_index("tm")
    peers = lax.axis_size("tm")
    seen = ((reach_ref[0, 0] == 1) & (place > 0), (reach_ref[0, 1] == 1) & (place < peers - 1))
    bias = [jnp.where(flag, 0.0, -1e30).astype(jnp.float32) for flag in seen]
    for h in range(q_ref.shape[1] // HD):
        at = slice(h * HD, (h + 1) * HD)
        query = q_ref[:, at]
        parts = []
        for ref, extra in ((kb_ref, bias[0]), (k_ref, None), (ka_ref, bias[1])):
            part = lax.dot_general(query, ref[:, at], (((1,), (1,)), ((), ())), preferred_element_type=jnp.float32)
            part = part * scale
            parts.append(part if extra is None else part + extra)
        top = functools.reduce(jnp.maximum, [jnp.max(part, axis=-1, keepdims=True) for part in parts])
        expo = [jnp.exp(part - top) for part in parts]
        total = functools.reduce(jnp.add, [jnp.sum(part, axis=-1, keepdims=True) for part in expo])
        share = 1.0 / total
        out = None
        for part, ref in zip(expo, (vb_ref, v_ref, va_ref)):
            weights = (part * share).astype(jnp.bfloat16)
            term = jnp.dot(weights, ref[:, at], preferred_element_type=jnp.float32)
            out = term if out is None else out + term
        o_ref[:, at] = out.astype(jnp.bfloat16)


def attend(reach, qn, pairs):
    rows, chans = qn.shape
    heads = chans // HD
    step = next(n for n in (5, 4, 3, 2, 1) if heads % n == 0)
    cols = step * HD
    steps = chans // cols
    k_spec = pl.BlockSpec((rows, cols), lambda i: (0, i))
    v_spec = pl.BlockSpec((rows, cols), lambda i: (0, steps + i))
    return pl.pallas_call(
        attend_kernel,
        grid=(steps,),
        out_shape=jax.ShapeDtypeStruct((rows, chans), jnp.bfloat16),
        in_specs=[pl.BlockSpec(memory_space=pltpu.SMEM)] + [k_spec] * 4 + [v_spec] * 3,
        out_specs=k_spec,
        name="attend",
    )(reach, qn, *pairs, *pairs)


def project_kernel(share, gate_ref, *refs):
    slots = len(refs) - 6
    att_refs, w_refs, outs = refs[:2], refs[2 : 2 + slots], refs[2 + slots : 4 + slots]
    w_ref, sems = refs[4 + slots :]
    depth, cols = w_refs[0].shape
    place = lax.axis_index("tm")
    line = place // 4
    copies = []
    for i, ref in enumerate(w_refs):
        start = pl.multiple_of((line ^ i) * depth, depth) if slots > 1 else 0
        copies.append(pltpu.make_async_copy(ref, w_ref.at[pl.ds(start, depth)], sems.at[i]))
    for copy in copies:
        copy.start()
    accs = [None, None]
    group = 2 if slots > 1 else 1
    for i in range(0, slots, group):
        for copy in copies[i : i + group]:
            copy.wait()
        start = pl.multiple_of((line // 2 ^ i // 2) * 2 * depth, HD) if slots > 1 else 0
        weight = w_ref[pl.ds(start, group * depth), :]
        for p in range(2):
            term = jnp.dot(att_refs[p][:, pl.ds(start, group * depth)], weight, preferred_element_type=jnp.float32)
            accs[p] = term if accs[p] is None else accs[p] + term
    first = ((place % 4) * 2 + (lax.axis_index("groups") ^ share)) * (cols // HD)
    for p in range(2):
        for b in range(cols // HD):
            at = slice(b * HD, (b + 1) * HD)
            outs[p][:, at] = (gate_ref[pl.ds(first + b, 1), :] * accs[p][:, at]).astype(jnp.bfloat16)


def project(gate, att, weights, share):
    rows, chans = att[0].shape
    cols = weights[0].shape[1]
    slots = len(weights)
    return pl.pallas_call(
        functools.partial(project_kernel, share),
        out_shape=[jax.ShapeDtypeStruct((rows, cols), jnp.bfloat16)] * 2,
        in_specs=whole(3) + [pl.BlockSpec(memory_space=pl.ANY)] * slots,
        out_specs=whole(2),
        scratch_shapes=[pltpu.VMEM((chans, cols), jnp.bfloat16), pltpu.SemaphoreType.DMA((slots,))],
    )(gate.reshape(-1, HD), *att, *weights)


def place_kernel(spots, aliased, *refs):
    pieces, out_ref, sems = refs[aliased:-2], refs[-2], refs[-1]
    cols = pieces[0].shape[1]
    low = lax.axis_index("tm") % 4
    group = lax.axis_index("groups")
    copies = []
    for i, (ref, (near, share)) in enumerate(zip(pieces, spots)):
        start = pl.multiple_of(((low ^ near) * 2 + (group ^ share)) * cols, HD)
        copies.append(pltpu.make_async_copy(ref, out_ref.at[:, pl.ds(start, cols)], sems.at[i]))
    for copy in copies:
        copy.start()
    for copy in copies:
        copy.wait()


def place_pieces(base, pieces, spots):
    rows, cols = pieces[0].shape
    anywhere = pl.BlockSpec(memory_space=pl.ANY)
    aliased = 0 if base is None else 1
    return pl.pallas_call(
        functools.partial(place_kernel, spots, aliased),
        out_shape=jax.ShapeDtypeStruct((rows, cols * 8), jnp.bfloat16),
        in_specs=[anywhere] * aliased + whole(len(pieces)),
        out_specs=anywhere,
        scratch_shapes=[pltpu.SemaphoreType.DMA((len(pieces),))],
        input_output_aliases={0: 0} if aliased else {},
    )(*([] if base is None else [base]), *pieces)


def local(queries, keys, values, q_gain, k_gain, out_weight, out_gate, reach):
    peers = lax.axis_size("tm")
    place = lax.axis_index("tm")
    group = lax.axis_index("groups")
    low = place % 4
    line = place // 4
    lines = peers // 4
    _, width = out_weight.shape
    cols = width // 8

    def swap(x, bits):
        return lax.ppermute(x, "tm", [(i, i ^ bits) for i in range(peers)])

    def group_swap(x):
        return lax.ppermute(x, "groups", [(0, 1), (1, 0)])

    def along(x, moves):
        return lax.ppermute(x, "tm", [(4 * a + i, 4 * b + i) for a, b in moves for i in range(4)])

    def send(x, pairs):
        return lax.ppermute(x, "tm", pairs)

    up = [(i, i + 1) for i in range(peers - 1)]
    down = [(j, i) for i, j in up]

    def choose(flag, a, b):
        return jnp.where(flag, a, b)

    def column(quarter, share):
        return (quarter * 2 + share) * cols

    def weight_part(quarter):
        return lax.dynamic_slice_in_dim(out_weight, column(quarter, group), cols, 1)

    cuts = lax.optimization_barrier([weight_part(low ^ i) for i in range(4)])
    parts = [cuts[0]] + [swap(cuts[i], i) for i in (1, 2, 3)]
    odd, upper = (low % 2) == 1, low >= 2
    halves = [
        jnp.concatenate([choose(odd, b, a), choose(odd, a, b)], axis=0)
        for a, b in ((parts[0], parts[1]), (parts[2], parts[3]))
    ]
    block = jnp.concatenate([choose(upper, halves[1], halves[0]), choose(upper, halves[0], halves[1])], axis=0)

    kv = pair(keys, values, k_gain)
    seen = [send(kv, up), kv, send(kv, down)]
    qn = norm(queries, q_gain)

    if lines == 4:
        middle = (line == 1) | (line == 2)
        near = along(block, ((0, 1), (1, 0), (2, 3), (3, 2)))
        across = along(block, ((1, 2), (2, 1)))
        across_far = along(near, ((1, 2), (2, 1)))
        edge = along(across, ((1, 0), (2, 3)))
        edge_far = along(across_far, ((1, 0), (2, 3)))
        second = choose(middle, across_far, edge)
        third = choose(middle, across, edge_far)
        slots = [block, near, second, third]
    else:
        members = [[z * 4 + i for z in range(lines)] for i in range(4)]
        slots = [lax.all_gather(block, "tm", axis_index_groups=members, axis=0, tiled=True)]
    shares = [slots, [group_swap(slot) for slot in slots]]

    own = attend(reach, qn, seen)
    over = swap(own, 2)
    here, there = [own, swap(own, 1)], [over, swap(over, 1)]
    pieces = {}
    for j in range(2):
        made = project(out_gate, here, shares[j], j)
        pieces[0, j], pieces[1, j] = made[0], swap(made[1], 1)
        made = project(out_gate, there, shares[j], j)
        pieces[2, j], pieces[3, j] = swap(made[0], 2), swap(made[1], 3)
    last = [(2, 1), (3, 1)]
    most = [spot for spot in pieces if spot not in last]
    out = place_pieces(None, [pieces[spot] for spot in most], most)
    return place_pieces(out, [pieces[spot] for spot in last], last)


def solution(mesh):
    return jax.shard_map(
        local,
        mesh=mesh,
        in_specs=(
            P(("groups", "tm"), None),
            P(("groups", "tm"), None),
            P(("groups", "tm"), None),
            P(),
            P(),
            P("tm", None),
            P(),
            P(("groups", "tm"), None),
        ),
        out_specs=P(("groups", "tm"), None),
        check_vma=False,
    )
```

```python
import functools

import jax
import jax.numpy as jnp
from jax import lax
from jax.experimental import pallas as pl
from jax.experimental.pallas import tpu as pltpu
from jax.sharding import PartitionSpec as P


HD = 128


def whole(count):
    return [pl.BlockSpec(memory_space=pltpu.VMEM)] * count


def scaled_heads(x_ref, gain_ref):
    block = x_ref[...].astype(jnp.float32)
    inverse = lax.rsqrt(jnp.mean(block * block, axis=-1, keepdims=True) + 1e-06)
    for i in range(x_ref.shape[1] // HD):
        piece = x_ref[:, i * HD : (i + 1) * HD].astype(jnp.float32)
        yield i, (piece * inverse * gain_ref[i : i + 1, :]).astype(jnp.bfloat16)


def norm_kernel(x_ref, gain_ref, out_ref):
    for i, piece in scaled_heads(x_ref, gain_ref):
        out_ref[:, i * HD : (i + 1) * HD] = piece


def pair_kernel(k_ref, v_ref, gain_ref, out_ref, kn_ref):
    chans = k_ref.shape[1]
    for i, piece in scaled_heads(k_ref, gain_ref):
        out_ref[:, i * HD : (i + 1) * HD] = piece
        kn_ref[:, i * HD : (i + 1) * HD] = piece
    out_ref[:, chans:] = v_ref[...]


def norm(x, gain):
    return pl.pallas_call(
        norm_kernel,
        out_shape=jax.ShapeDtypeStruct(x.shape, jnp.bfloat16),
        in_specs=whole(2),
        out_specs=pl.BlockSpec(memory_space=pltpu.VMEM),
    )(x, gain.reshape(-1, HD))


def pair(keys, values, gain):
    rows, chans = keys.shape
    return pl.pallas_call(
        pair_kernel,
        out_shape=[jax.ShapeDtypeStruct((rows, n * chans), jnp.bfloat16) for n in (2, 1)],
        in_specs=whole(3),
        out_specs=whole(2),
    )(keys, values, gain.reshape(-1, HD))


def attend_kernel(reach_ref, q_ref, kb_ref, k_ref, ka_ref, vb_ref, v_ref, va_ref, kd_ref, vd_ref, o_ref):
    scale = HD ** (-0.5)
    place = lax.axis_index("tm")
    peers = lax.axis_size("tm")
    seen = ((reach_ref[0, 0] == 1) & (place > 0), (reach_ref[0, 1] == 1) & (place < peers - 1))
    bias = [jnp.where(flag, 0.0, -1e30).astype(jnp.float32) for flag in seen]
    low = place % 4

    def three(before_ref, own_ref, after_ref, other_ref, at):
        other = other_ref[:, at]
        before = jnp.where(low == 0, other, before_ref[:, at])
        return before, own_ref[:, at], jnp.where(low == 3, other, after_ref[:, at])

    for h in range(q_ref.shape[1] // HD):
        at = slice(h * HD, (h + 1) * HD)
        query = q_ref[:, at]
        parts = []
        for key, extra in zip(three(kb_ref, k_ref, ka_ref, kd_ref, at), (bias[0], None, bias[1])):
            part = lax.dot_general(query, key, (((1,), (1,)), ((), ())), preferred_element_type=jnp.float32)
            part = part * scale
            parts.append(part if extra is None else part + extra)
        top = functools.reduce(jnp.maximum, [jnp.max(part, axis=-1, keepdims=True) for part in parts])
        expo = [jnp.exp(part - top) for part in parts]
        total = functools.reduce(jnp.add, [jnp.sum(part, axis=-1, keepdims=True) for part in expo])
        share = 1.0 / total
        out = None
        for part, value in zip(expo, three(vb_ref, v_ref, va_ref, vd_ref, at)):
            weights = (part * share).astype(jnp.bfloat16)
            term = jnp.dot(weights, value, preferred_element_type=jnp.float32)
            out = term if out is None else out + term
        o_ref[:, at] = out.astype(jnp.bfloat16)


def attend(reach, qn, pairs, k_diag, v_diag):
    rows, chans = qn.shape
    heads = chans // HD
    step = next(n for n in (5, 4, 3, 2, 1) if heads % n == 0)
    cols = step * HD
    steps = chans // cols
    k_spec = pl.BlockSpec((rows, cols), lambda i: (0, i))
    v_spec = pl.BlockSpec((rows, cols), lambda i: (0, steps + i))
    return pl.pallas_call(
        attend_kernel,
        grid=(steps,),
        out_shape=jax.ShapeDtypeStruct((rows, chans), jnp.bfloat16),
        in_specs=[pl.BlockSpec(memory_space=pltpu.SMEM)] + [k_spec] * 4 + [v_spec] * 3 + [k_spec] * 2,
        out_specs=k_spec,
        name="attend",
    )(reach, qn, *pairs, *pairs, k_diag, v_diag)


def project_kernel(share, gate_ref, *refs):
    slots = len(refs) - 6
    att_refs, w_refs, outs = refs[:2], refs[2 : 2 + slots], refs[2 + slots : 4 + slots]
    w_ref, sems = refs[4 + slots :]
    depth, cols = w_refs[0].shape
    place = lax.axis_index("tm")
    line = place // 4
    copies = []
    for i, ref in enumerate(w_refs):
        start = pl.multiple_of((line ^ i) * depth, depth) if slots > 1 else 0
        copies.append(pltpu.make_async_copy(ref, w_ref.at[pl.ds(start, depth)], sems.at[i]))
    for copy in copies:
        copy.start()
    rows = att_refs[0].shape[0]
    acc = None
    group = 2 if slots > 1 else 1
    for i in range(0, slots, group):
        for copy in copies[i : i + group]:
            copy.wait()
        start = pl.multiple_of((line // 2 ^ i // 2) * 2 * depth, HD) if slots > 1 else 0
        weight = w_ref[pl.ds(start, group * depth), :]
        both = jnp.concatenate([ref[:, pl.ds(start, group * depth)] for ref in att_refs], axis=0)
        term = jnp.dot(both, weight, preferred_element_type=jnp.float32)
        acc = term if acc is None else acc + term
    first = ((place % 4) * 2 + (lax.axis_index("groups") ^ share)) * (cols // HD)
    for p in range(2):
        for b in range(cols // HD):
            at = slice(b * HD, (b + 1) * HD)
            outs[p][:, at] = (gate_ref[pl.ds(first + b, 1), :] * acc[p * rows : (p + 1) * rows, at]).astype(jnp.bfloat16)


def project(gate, att, weights, share):
    rows, chans = att[0].shape
    cols = weights[0].shape[1]
    slots = len(weights)
    return pl.pallas_call(
        functools.partial(project_kernel, share),
        out_shape=[jax.ShapeDtypeStruct((rows, cols), jnp.bfloat16)] * 2,
        in_specs=whole(3) + [pl.BlockSpec(memory_space=pl.ANY)] * slots,
        out_specs=whole(2),
        scratch_shapes=[pltpu.VMEM((chans, cols), jnp.bfloat16), pltpu.SemaphoreType.DMA((slots,))],
    )(gate.reshape(-1, HD), *att, *weights)


def place_kernel(spots, aliased, *refs):
    pieces, out_ref, sems = refs[aliased:-2], refs[-2], refs[-1]
    cols = pieces[0].shape[1]
    low = lax.axis_index("tm") % 4
    group = lax.axis_index("groups")
    copies = []
    for i, (ref, (near, share)) in enumerate(zip(pieces, spots)):
        start = pl.multiple_of(((low ^ near) * 2 + (group ^ share)) * cols, HD)
        copies.append(pltpu.make_async_copy(ref, out_ref.at[:, pl.ds(start, cols)], sems.at[i]))
    for copy in copies:
        copy.start()
    for copy in copies:
        copy.wait()


def place_pieces(base, pieces, spots):
    rows, cols = pieces[0].shape
    anywhere = pl.BlockSpec(memory_space=pl.ANY)
    aliased = 0 if base is None else 1
    return pl.pallas_call(
        functools.partial(place_kernel, spots, aliased),
        out_shape=jax.ShapeDtypeStruct((rows, cols * 8), jnp.bfloat16),
        in_specs=[anywhere] * aliased + whole(len(pieces)),
        out_specs=anywhere,
        scratch_shapes=[pltpu.SemaphoreType.DMA((len(pieces),))],
        input_output_aliases={0: 0} if aliased else {},
    )(*([] if base is None else [base]), *pieces)


def local(queries, keys, values, q_gain, k_gain, out_weight, out_gate, reach):
    peers = lax.axis_size("tm")
    place = lax.axis_index("tm")
    group = lax.axis_index("groups")
    low = place % 4
    line = place // 4
    lines = peers // 4
    _, width = out_weight.shape
    cols = width // 8

    def swap(x, bits):
        return lax.ppermute(x, "tm", [(i, i ^ bits) for i in range(peers)])

    def group_swap(x):
        return lax.ppermute(x, "groups", [(0, 1), (1, 0)])

    def along(x, moves):
        return lax.ppermute(x, "tm", [(4 * a + i, 4 * b + i) for a, b in moves for i in range(4)])

    def send(x, pairs):
        return lax.ppermute(x, "tm", pairs)

    up = [(i, i + 1) for i in range(peers - 1)]
    down = [(j, i) for i, j in up]

    def inside(pairs):
        return [(i, j) for i, j in pairs if i // 4 == j // 4]

    def outside(pairs):
        return [(i, j) for i, j in pairs if i // 4 != j // 4]

    def choose(flag, a, b):
        return jnp.where(flag, a, b)

    def column(quarter, share):
        return (quarter * 2 + share) * cols

    def weight_part(quarter):
        return lax.dynamic_slice_in_dim(out_weight, column(quarter, group), cols, 1)

    cuts = lax.optimization_barrier([weight_part(low ^ i) for i in range(4)])
    parts = [cuts[0]] + [swap(cuts[i], i) for i in (1, 2, 3)]
    odd, upper = (low % 2) == 1, low >= 2
    halves = [
        jnp.concatenate([choose(odd, b, a), choose(odd, a, b)], axis=0)
        for a, b in ((parts[0], parts[1]), (parts[2], parts[3]))
    ]
    block = jnp.concatenate([choose(upper, halves[1], halves[0]), choose(upper, halves[0], halves[1])], axis=0)

    kv, kn = pair(keys, values, k_gain)
    near = [send(kv, inside(up)), kv, send(kv, inside(down))]
    k_diag = send(kn, outside(up) + outside(down))
    turn = [(4 * z + i, 4 * z + (i ^ 2)) for z in range(lines) for i in (0, 3)]
    leap = [(i ^ 2, j) for i, j in outside(up) + outside(down)]
    v_diag = send(send(values, turn), leap)
    qn = norm(queries, q_gain)

    if lines == 4:
        middle = (line == 1) | (line == 2)
        beside = along(block, ((0, 1), (1, 0), (2, 3), (3, 2)))
        across = along(block, ((1, 2), (2, 1)))
        across_far = along(beside, ((1, 2), (2, 1)))
        edge = along(across, ((1, 0), (2, 3)))
        edge_far = along(across_far, ((1, 0), (2, 3)))
        second = choose(middle, across_far, edge)
        third = choose(middle, across, edge_far)
        slots = [block, beside, second, third]
    else:
        members = [[z * 4 + i for z in range(lines)] for i in range(4)]
        slots = [lax.all_gather(block, "tm", axis_index_groups=members, axis=0, tiled=True)]
    shares = [slots, [group_swap(slot) for slot in slots]]

    own = attend(reach, qn, near, k_diag, v_diag)
    over = swap(own, 2)
    here, there = [own, swap(own, 1)], [over, swap(over, 1)]
    pieces = {}
    for j in range(2):
        made = project(out_gate, here, shares[j], j)
        pieces[0, j], pieces[1, j] = made[0], swap(made[1], 1)
        made = project(out_gate, there, shares[j], j)
        pieces[2, j], pieces[3, j] = swap(made[0], 2), swap(made[1], 3)
    last = [(2, 1), (3, 1)]
    most = [spot for spot in pieces if spot not in last]
    out = place_pieces(None, [pieces[spot] for spot in most], most)
    return place_pieces(out, [pieces[spot] for spot in last], last)


def solution(mesh):
    return jax.shard_map(
        local,
        mesh=mesh,
        in_specs=(
            P(("groups", "tm"), None),
            P(("groups", "tm"), None),
            P(("groups", "tm"), None),
            P(),
            P(),
            P("tm", None),
            P(),
            P(("groups", "tm"), None),
        ),
        out_specs=P(("groups", "tm"), None),
        check_vma=False,
    )
```

```python
import functools

import jax
import jax.numpy as jnp
from jax import lax
from jax.experimental import pallas as pl
from jax.experimental.pallas import tpu as pltpu
from jax.sharding import PartitionSpec as P


HD = 128


def whole(count):
    return [pl.BlockSpec(memory_space=pltpu.VMEM)] * count


def scaled_heads(x_ref, gain_ref):
    block = x_ref[...].astype(jnp.float32)
    inverse = lax.rsqrt(jnp.mean(block * block, axis=-1, keepdims=True) + 1e-06)
    for i in range(x_ref.shape[1] // HD):
        piece = x_ref[:, i * HD : (i + 1) * HD].astype(jnp.float32)
        yield i, (piece * inverse * gain_ref[i : i + 1, :]).astype(jnp.bfloat16)


def norm_kernel(x_ref, gain_ref, out_ref):
    for i, piece in scaled_heads(x_ref, gain_ref):
        out_ref[:, i * HD : (i + 1) * HD] = piece


def pair_kernel(k_ref, v_ref, gain_ref, out_ref, kn_ref):
    chans = k_ref.shape[1]
    for i, piece in scaled_heads(k_ref, gain_ref):
        out_ref[:, i * HD : (i + 1) * HD] = piece
        kn_ref[:, i * HD : (i + 1) * HD] = piece
    out_ref[:, chans:] = v_ref[...]


def norm(x, gain):
    return pl.pallas_call(
        norm_kernel,
        out_shape=jax.ShapeDtypeStruct(x.shape, jnp.bfloat16),
        in_specs=whole(2),
        out_specs=pl.BlockSpec(memory_space=pltpu.VMEM),
    )(x, gain.reshape(-1, HD))


def pair(keys, values, gain):
    rows, chans = keys.shape
    return pl.pallas_call(
        pair_kernel,
        out_shape=[jax.ShapeDtypeStruct((rows, n * chans), jnp.bfloat16) for n in (2, 1)],
        in_specs=whole(3),
        out_specs=whole(2),
    )(keys, values, gain.reshape(-1, HD))


def attend_kernel(reach_ref, q_ref, kb_ref, k_ref, ka_ref, vb_ref, v_ref, va_ref, kd_ref, vd_ref, o_ref):
    scale = HD ** (-0.5)
    place = lax.axis_index("tm")
    peers = lax.axis_size("tm")
    seen = ((reach_ref[0, 0] == 1) & (place > 0), (reach_ref[0, 1] == 1) & (place < peers - 1))
    bias = [jnp.where(flag, 0.0, -1e30).astype(jnp.float32) for flag in seen]
    low = place % 4

    def three(before_ref, own_ref, after_ref, other_ref, at):
        other = other_ref[:, at]
        before = jnp.where(low == 0, other, before_ref[:, at])
        return before, own_ref[:, at], jnp.where(low == 3, other, after_ref[:, at])

    for h in range(q_ref.shape[1] // HD):
        at = slice(h * HD, (h + 1) * HD)
        query = q_ref[:, at]
        parts = []
        for key, extra in zip(three(kb_ref, k_ref, ka_ref, kd_ref, at), (bias[0], None, bias[1])):
            part = lax.dot_general(query, key, (((1,), (1,)), ((), ())), preferred_element_type=jnp.float32)
            part = part * scale
            parts.append(part if extra is None else part + extra)
        top = functools.reduce(jnp.maximum, [jnp.max(part, axis=-1, keepdims=True) for part in parts])
        expo = [jnp.exp(part - top) for part in parts]
        total = functools.reduce(jnp.add, [jnp.sum(part, axis=-1, keepdims=True) for part in expo])
        share = 1.0 / total
        out = None
        for part, value in zip(expo, three(vb_ref, v_ref, va_ref, vd_ref, at)):
            weights = (part * share).astype(jnp.bfloat16)
            term = jnp.dot(weights, value, preferred_element_type=jnp.float32)
            out = term if out is None else out + term
        o_ref[:, at] = out.astype(jnp.bfloat16)


def attend(reach, qn, pairs, k_diag, v_diag, chunk, chunks):
    rows, chans = qn.shape
    wide = chans // chunks
    heads = wide // HD
    step = next(n for n in (5, 4, 3, 2, 1) if heads % n == 0)
    cols = step * HD
    steps = wide // cols
    k_spec = pl.BlockSpec((rows, cols), lambda i: (0, chunk * steps + i))
    v_spec = pl.BlockSpec((rows, cols), lambda i: (0, (chunks + chunk) * steps + i))
    return pl.pallas_call(
        attend_kernel,
        grid=(steps,),
        out_shape=jax.ShapeDtypeStruct((rows, wide), jnp.bfloat16),
        in_specs=[pl.BlockSpec(memory_space=pltpu.SMEM)] + [k_spec] * 4 + [v_spec] * 3 + [k_spec] * 2,
        out_specs=pl.BlockSpec((rows, cols), lambda i: (0, i)),
    )(reach, qn, *pairs, *pairs, k_diag, v_diag)


def project_kernel(share, count, gate_ref, *refs):
    slots = len(refs) - count - 3
    att_refs, w_refs, outs = refs[:count], refs[count : count + slots], refs[-3:-1]
    a_ref = refs[-1]
    rows, wide = att_refs[0].shape
    depth, cols = w_refs[0].shape
    chunks = count // 2
    place = lax.axis_index("tm")
    line = place // 4
    for i, ref in enumerate(att_refs):
        p, j = i // chunks, i % chunks
        a_ref[p * rows : (p + 1) * rows, j * wide : (j + 1) * wide] = ref[...]
    acc = None
    for i, ref in enumerate(w_refs):
        start = pl.multiple_of((line ^ i) * depth, HD) if slots > 1 else 0
        term = jnp.dot(a_ref[:, pl.ds(start, depth)], ref[...], preferred_element_type=jnp.float32)
        acc = term if acc is None else acc + term
    first = ((place % 4) * 2 + (lax.axis_index("groups") ^ share)) * (cols // HD)
    for p in range(2):
        for b in range(cols // HD):
            at = slice(b * HD, (b + 1) * HD)
            scaled = gate_ref[pl.ds(first + b, 1), :] * acc[p * rows : (p + 1) * rows, at]
            outs[p][:, at] = scaled.astype(jnp.bfloat16)


def project(gate, att, weights, share):
    rows, wide = att[0].shape
    cols = weights[0].shape[1]
    return pl.pallas_call(
        functools.partial(project_kernel, share, len(att)),
        out_shape=[jax.ShapeDtypeStruct((rows, cols), jnp.bfloat16)] * 2,
        in_specs=whole(1 + len(att) + len(weights)),
        out_specs=whole(2),
        scratch_shapes=[pltpu.VMEM((2 * rows, wide * len(att) // 2), jnp.bfloat16)],
    )(gate.reshape(-1, HD), *att, *weights)


def place_kernel(spots, aliased, *refs):
    pieces, out_ref, sems = refs[aliased:-2], refs[-2], refs[-1]
    cols = pieces[0].shape[1]
    low = lax.axis_index("tm") % 4
    group = lax.axis_index("groups")
    copies = []
    for i, (ref, (near, share)) in enumerate(zip(pieces, spots)):
        start = pl.multiple_of(((low ^ near) * 2 + (group ^ share)) * cols, HD)
        copies.append(pltpu.make_async_copy(ref, out_ref.at[:, pl.ds(start, cols)], sems.at[i]))
    for copy in copies:
        copy.start()
    for copy in copies:
        copy.wait()


def place_pieces(base, pieces, spots):
    rows, cols = pieces[0].shape
    anywhere = pl.BlockSpec(memory_space=pl.ANY)
    aliased = 0 if base is None else 1
    return pl.pallas_call(
        functools.partial(place_kernel, spots, aliased),
        out_shape=jax.ShapeDtypeStruct((rows, cols * 8), jnp.bfloat16),
        in_specs=[anywhere] * aliased + whole(len(pieces)),
        out_specs=anywhere,
        scratch_shapes=[pltpu.SemaphoreType.DMA((len(pieces),))],
        input_output_aliases={0: 0} if aliased else {},
    )(*([] if base is None else [base]), *pieces)


def local(queries, keys, values, q_gain, k_gain, out_weight, out_gate, reach):
    peers = lax.axis_size("tm")
    place = lax.axis_index("tm")
    group = lax.axis_index("groups")
    low = place % 4
    line = place // 4
    lines = peers // 4
    _, width = out_weight.shape
    _, chans = queries.shape
    cols = width // 8
    chunks = 2 if chans // HD % 2 == 0 else 1

    def swap(x, bits):
        return lax.ppermute(x, "tm", [(i, i ^ bits) for i in range(peers)])

    def group_swap(x):
        return lax.ppermute(x, "groups", [(0, 1), (1, 0)])

    def along(x, moves):
        return lax.ppermute(x, "tm", [(4 * a + i, 4 * b + i) for a, b in moves for i in range(4)])

    def send(x, pairs):
        return lax.ppermute(x, "tm", pairs)

    up = [(i, i + 1) for i in range(peers - 1)]
    down = [(j, i) for i, j in up]

    def inside(pairs):
        return [(i, j) for i, j in pairs if i // 4 == j // 4]

    def outside(pairs):
        return [(i, j) for i, j in pairs if i // 4 != j // 4]

    def choose(flag, a, b):
        return jnp.where(flag, a, b)

    def column(quarter, share):
        return (quarter * 2 + share) * cols

    def weight_part(quarter):
        return lax.dynamic_slice_in_dim(out_weight, column(quarter, group), cols, 1)

    cuts = lax.optimization_barrier([weight_part(low ^ i) for i in range(4)])
    parts = [cuts[0]] + [swap(cuts[i], i) for i in (1, 2, 3)]
    odd, upper = (low % 2) == 1, low >= 2
    halves = [
        jnp.concatenate([choose(odd, b, a), choose(odd, a, b)], axis=0)
        for a, b in ((parts[0], parts[1]), (parts[2], parts[3]))
    ]
    block = jnp.concatenate([choose(upper, halves[1], halves[0]), choose(upper, halves[0], halves[1])], axis=0)

    kv, kn = pair(keys, values, k_gain)
    near = [send(kv, inside(up)), kv, send(kv, inside(down))]
    k_diag = send(kn, outside(up) + outside(down))
    turn = [(4 * z + i, 4 * z + (i ^ 2)) for z in range(lines) for i in (0, 3)]
    leap = [(i ^ 2, j) for i, j in outside(up) + outside(down)]
    v_diag = send(send(values, turn), leap)
    qn = norm(queries, q_gain)

    if lines == 4:
        middle = (line == 1) | (line == 2)
        beside = along(block, ((0, 1), (1, 0), (2, 3), (3, 2)))
        across = along(block, ((1, 2), (2, 1)))
        across_far = along(beside, ((1, 2), (2, 1)))
        edge = along(across, ((1, 0), (2, 3)))
        edge_far = along(across_far, ((1, 0), (2, 3)))
        second = choose(middle, across_far, edge)
        third = choose(middle, across, edge_far)
        slots = [block, beside, second, third]
    else:
        members = [[z * 4 + i for z in range(lines)] for i in range(4)]
        slots = [lax.all_gather(block, "tm", axis_index_groups=members, axis=0, tiled=True)]
    shares = [slots, [group_swap(slot) for slot in slots]]

    here, there = [], []
    for i in range(chunks):
        own = attend(reach, qn, near, k_diag, v_diag, i, chunks)
        over = swap(own, 2)
        here.append([own, swap(own, 1)])
        there.append([over, swap(over, 1)])
    here = [pair[p] for p in range(2) for pair in here]
    there = [pair[p] for p in range(2) for pair in there]
    pieces = {}
    for j in range(2):
        made = project(out_gate, here, shares[j], j)
        pieces[0, j], pieces[1, j] = made[0], swap(made[1], 1)
        made = project(out_gate, there, shares[j], j)
        pieces[2, j], pieces[3, j] = swap(made[0], 2), swap(made[1], 3)
    last = [(2, 1), (3, 1)]
    most = [spot for spot in pieces if spot not in last]
    out = place_pieces(None, [pieces[spot] for spot in most], most)
    return place_pieces(out, [pieces[spot] for spot in last], last)


def solution(mesh):
    return jax.shard_map(
        local,
        mesh=mesh,
        in_specs=(
            P(("groups", "tm"), None),
            P(("groups", "tm"), None),
            P(("groups", "tm"), None),
            P(),
            P(),
            P("tm", None),
            P(),
            P(("groups", "tm"), None),
        ),
        out_specs=P(("groups", "tm"), None),
        check_vma=False,
    )
```

```python
import functools

import jax
import jax.numpy as jnp
from jax import lax
from jax.experimental import pallas as pl
from jax.experimental.pallas import tpu as pltpu
from jax.sharding import PartitionSpec as P


HD = 128


LIMIT = pltpu.CompilerParams(vmem_limit_bytes=16 * 1024 * 1024)


def whole(count):
    return [pl.BlockSpec(memory_space=pltpu.VMEM)] * count


def scaled_heads(x_ref, gain_ref):
    block = x_ref[...].astype(jnp.float32)
    inverse = lax.rsqrt(jnp.mean(block * block, axis=-1, keepdims=True) + 1e-06)
    for i in range(x_ref.shape[1] // HD):
        piece = x_ref[:, i * HD : (i + 1) * HD].astype(jnp.float32)
        yield i, (piece * inverse * gain_ref[i : i + 1, :]).astype(jnp.bfloat16)


def norm_kernel(x_ref, gain_ref, out_ref):
    for i, piece in scaled_heads(x_ref, gain_ref):
        out_ref[:, i * HD : (i + 1) * HD] = piece


def pair_kernel(k_ref, v_ref, gain_ref, out_ref, kn_ref):
    chans = k_ref.shape[1]
    for i, piece in scaled_heads(k_ref, gain_ref):
        out_ref[:, i * HD : (i + 1) * HD] = piece
        kn_ref[:, i * HD : (i + 1) * HD] = piece
    out_ref[:, chans:] = v_ref[...]


def norm(x, gain):
    return pl.pallas_call(
        norm_kernel,
        out_shape=jax.ShapeDtypeStruct(x.shape, jnp.bfloat16),
        in_specs=whole(2),
        out_specs=pl.BlockSpec(memory_space=pltpu.VMEM),
        compiler_params=LIMIT,
    )(x, gain.reshape(-1, HD))


def pair(keys, values, gain):
    rows, chans = keys.shape
    return pl.pallas_call(
        pair_kernel,
        out_shape=[jax.ShapeDtypeStruct((rows, n * chans), jnp.bfloat16) for n in (2, 1)],
        in_specs=whole(3),
        out_specs=whole(2),
        compiler_params=LIMIT,
    )(keys, values, gain.reshape(-1, HD))


def attend_kernel(reach_ref, q_ref, kb_ref, k_ref, ka_ref, vb_ref, v_ref, va_ref, kd_ref, vd_ref, o_ref):
    scale = HD ** (-0.5)
    place = lax.axis_index("tm")
    peers = lax.axis_size("tm")
    seen = ((reach_ref[0, 0] == 1) & (place > 0), (reach_ref[0, 1] == 1) & (place < peers - 1))
    bias = [jnp.where(flag, 0.0, -1e30).astype(jnp.float32) for flag in seen]
    low = place % 4

    def three(before_ref, own_ref, after_ref, other_ref, at):
        other = other_ref[:, at]
        before = jnp.where(low == 0, other, before_ref[:, at])
        return before, own_ref[:, at], jnp.where(low == 3, other, after_ref[:, at])

    for h in range(q_ref.shape[1] // HD):
        at = slice(h * HD, (h + 1) * HD)
        query = q_ref[:, at]
        parts = []
        for key, extra in zip(three(kb_ref, k_ref, ka_ref, kd_ref, at), (bias[0], None, bias[1])):
            part = lax.dot_general(query, key, (((1,), (1,)), ((), ())), preferred_element_type=jnp.float32)
            part = part * scale
            parts.append(part if extra is None else part + extra)
        top = functools.reduce(jnp.maximum, [jnp.max(part, axis=-1, keepdims=True) for part in parts])
        expo = [jnp.exp(part - top) for part in parts]
        total = functools.reduce(jnp.add, [jnp.sum(part, axis=-1, keepdims=True) for part in expo])
        share = 1.0 / total
        out = None
        for part, value in zip(expo, three(vb_ref, v_ref, va_ref, vd_ref, at)):
            weights = (part * share).astype(jnp.bfloat16)
            term = jnp.dot(weights, value, preferred_element_type=jnp.float32)
            out = term if out is None else out + term
        o_ref[:, at] = out.astype(jnp.bfloat16)


def attend(reach, qn, pairs, k_diag, v_diag, chunk, chunks):
    rows, chans = qn.shape
    wide = chans // chunks
    heads = wide // HD
    step = next(n for n in (5, 4, 3, 2, 1) if heads % n == 0)
    cols = step * HD
    steps = wide // cols
    k_spec = pl.BlockSpec((rows, cols), lambda i: (0, chunk * steps + i))
    v_spec = pl.BlockSpec((rows, cols), lambda i: (0, (chunks + chunk) * steps + i))
    return pl.pallas_call(
        attend_kernel,
        grid=(steps,),
        out_shape=jax.ShapeDtypeStruct((rows, wide), jnp.bfloat16),
        in_specs=[pl.BlockSpec(memory_space=pltpu.SMEM)] + [k_spec] * 4 + [v_spec] * 3 + [k_spec] * 2,
        out_specs=pl.BlockSpec((rows, cols), lambda i: (0, i)),
        compiler_params=LIMIT,
    )(reach, qn, *pairs, *pairs, k_diag, v_diag)


def project_kernel(share, count, gate_ref, *refs):
    slots = len(refs) - count - 3
    att_refs, w_refs, outs = refs[:count], refs[count : count + slots], refs[-3:-1]
    a_ref = refs[-1]
    rows, wide = att_refs[0].shape
    depth, cols = w_refs[0].shape
    chunks = count // 2
    place = lax.axis_index("tm")
    line = place // 4
    for i, ref in enumerate(att_refs):
        p, j = i // chunks, i % chunks
        a_ref[p * rows : (p + 1) * rows, j * wide : (j + 1) * wide] = ref[...]
    acc = None
    for i, ref in enumerate(w_refs):
        start = pl.multiple_of((line ^ i) * depth, HD) if slots > 1 else 0
        term = jnp.dot(a_ref[:, pl.ds(start, depth)], ref[...], preferred_element_type=jnp.float32)
        acc = term if acc is None else acc + term
    first = ((place % 4) * 2 + (lax.axis_index("groups") ^ share)) * (cols // HD)
    for p in range(2):
        for b in range(cols // HD):
            at = slice(b * HD, (b + 1) * HD)
            scaled = gate_ref[pl.ds(first + b, 1), :] * acc[p * rows : (p + 1) * rows, at]
            outs[p][:, at] = scaled.astype(jnp.bfloat16)


def project(gate, att, weights, share):
    rows, wide = att[0].shape
    cols = weights[0].shape[1]
    return pl.pallas_call(
        functools.partial(project_kernel, share, len(att)),
        out_shape=[jax.ShapeDtypeStruct((rows, cols), jnp.bfloat16)] * 2,
        in_specs=whole(1 + len(att) + len(weights)),
        out_specs=whole(2),
        scratch_shapes=[pltpu.VMEM((2 * rows, wide * len(att) // 2), jnp.bfloat16)],
        compiler_params=LIMIT,
    )(gate.reshape(-1, HD), *att, *weights)


def place_kernel(spots, aliased, *refs):
    pieces, out_ref, sems = refs[aliased:-2], refs[-2], refs[-1]
    cols = pieces[0].shape[1]
    low = lax.axis_index("tm") % 4
    group = lax.axis_index("groups")
    copies = []
    for i, (ref, (near, share)) in enumerate(zip(pieces, spots)):
        start = pl.multiple_of(((low ^ near) * 2 + (group ^ share)) * cols, HD)
        copies.append(pltpu.make_async_copy(ref, out_ref.at[:, pl.ds(start, cols)], sems.at[i]))
    for copy in copies:
        copy.start()
    for copy in copies:
        copy.wait()


def place_pieces(base, pieces, spots):
    rows, cols = pieces[0].shape
    anywhere = pl.BlockSpec(memory_space=pl.ANY)
    aliased = 0 if base is None else 1
    return pl.pallas_call(
        functools.partial(place_kernel, spots, aliased),
        out_shape=jax.ShapeDtypeStruct((rows, cols * 8), jnp.bfloat16),
        in_specs=[anywhere] * aliased + whole(len(pieces)),
        out_specs=anywhere,
        scratch_shapes=[pltpu.SemaphoreType.DMA((len(pieces),))],
        input_output_aliases={0: 0} if aliased else {},
        compiler_params=LIMIT,
    )(*([] if base is None else [base]), *pieces)


def local(queries, keys, values, q_gain, k_gain, out_weight, out_gate, reach):
    peers = lax.axis_size("tm")
    place = lax.axis_index("tm")
    group = lax.axis_index("groups")
    low = place % 4
    line = place // 4
    lines = peers // 4
    _, width = out_weight.shape
    _, chans = queries.shape
    cols = width // 8
    chunks = 2 if chans // HD % 2 == 0 else 1

    def swap(x, bits):
        return lax.ppermute(x, "tm", [(i, i ^ bits) for i in range(peers)])

    def group_swap(x):
        return lax.ppermute(x, "groups", [(0, 1), (1, 0)])

    def along(x, moves):
        return lax.ppermute(x, "tm", [(4 * a + i, 4 * b + i) for a, b in moves for i in range(4)])

    def send(x, pairs):
        return lax.ppermute(x, "tm", pairs)

    up = [(i, i + 1) for i in range(peers - 1)]
    down = [(j, i) for i, j in up]

    def inside(pairs):
        return [(i, j) for i, j in pairs if i // 4 == j // 4]

    def outside(pairs):
        return [(i, j) for i, j in pairs if i // 4 != j // 4]

    def choose(flag, a, b):
        return jnp.where(flag, a, b)

    def column(quarter, share):
        return (quarter * 2 + share) * cols

    def weight_part(quarter):
        return lax.dynamic_slice_in_dim(out_weight, column(quarter, group), cols, 1)

    cuts = lax.optimization_barrier([weight_part(low ^ i) for i in range(4)])
    parts = [cuts[0]] + [swap(cuts[i], i) for i in (1, 2, 3)]
    odd, upper = (low % 2) == 1, low >= 2
    halves = [
        jnp.concatenate([choose(odd, b, a), choose(odd, a, b)], axis=0)
        for a, b in ((parts[0], parts[1]), (parts[2], parts[3]))
    ]
    block = jnp.concatenate([choose(upper, halves[1], halves[0]), choose(upper, halves[0], halves[1])], axis=0)

    kv, kn = pair(keys, values, k_gain)
    near = [send(kv, inside(up)), kv, send(kv, inside(down))]
    k_diag = send(kn, outside(up) + outside(down))
    turn = [(4 * z + i, 4 * z + (i ^ 2)) for z in range(lines) for i in (0, 3)]
    leap = [(i ^ 2, j) for i, j in outside(up) + outside(down)]
    v_diag = send(send(values, turn), leap)
    qn = norm(queries, q_gain)

    if lines == 4:
        middle = (line == 1) | (line == 2)
        beside = along(block, ((0, 1), (1, 0), (2, 3), (3, 2)))
        across = along(block, ((1, 2), (2, 1)))
        across_far = along(beside, ((1, 2), (2, 1)))
        edge = along(across, ((1, 0), (2, 3)))
        edge_far = along(across_far, ((1, 0), (2, 3)))
        second = choose(middle, across_far, edge)
        third = choose(middle, across, edge_far)
        slots = [block, beside, second, third]
    else:
        members = [[z * 4 + i for z in range(lines)] for i in range(4)]
        slots = [lax.all_gather(block, "tm", axis_index_groups=members, axis=0, tiled=True)]
    shares = [slots, [group_swap(slot) for slot in slots]]

    here, there = [], []
    for i in range(chunks):
        own = attend(reach, qn, near, k_diag, v_diag, i, chunks)
        over = swap(own, 2)
        here.append([own, swap(own, 1)])
        there.append([over, swap(over, 1)])
    here = [pair[p] for p in range(2) for pair in here]
    there = [pair[p] for p in range(2) for pair in there]
    pieces = {}
    for j in range(2):
        made = project(out_gate, here, shares[j], j)
        pieces[0, j], pieces[1, j] = made[0], swap(made[1], 1)
        made = project(out_gate, there, shares[j], j)
        pieces[2, j], pieces[3, j] = swap(made[0], 2), swap(made[1], 3)
    last = [(2, 1), (3, 1)]
    most = [spot for spot in pieces if spot not in last]
    out = place_pieces(None, [pieces[spot] for spot in most], most)
    return place_pieces(out, [pieces[spot] for spot in last], last)


def solution(mesh):
    return jax.shard_map(
        local,
        mesh=mesh,
        in_specs=(
            P(("groups", "tm"), None),
            P(("groups", "tm"), None),
            P(("groups", "tm"), None),
            P(),
            P(),
            P("tm", None),
            P(),
            P(("groups", "tm"), None),
        ),
        out_specs=P(("groups", "tm"), None),
        check_vma=False,
    )
```

```python
import functools

import jax
import jax.numpy as jnp
from jax import lax
from jax.experimental import pallas as pl
from jax.experimental.pallas import tpu as pltpu
from jax.sharding import PartitionSpec as P


HD = 128


LIMIT = pltpu.CompilerParams(vmem_limit_bytes=16 * 1024 * 1024)


def whole(count):
    return [pl.BlockSpec(memory_space=pltpu.VMEM)] * count


def scaled_heads(x_ref, gain_ref):
    block = x_ref[...].astype(jnp.float32)
    inverse = lax.rsqrt(jnp.mean(block * block, axis=-1, keepdims=True) + 1e-06)
    for i in range(x_ref.shape[1] // HD):
        piece = x_ref[:, i * HD : (i + 1) * HD].astype(jnp.float32)
        yield i, (piece * inverse * gain_ref[i : i + 1, :]).astype(jnp.bfloat16)


def norm_kernel(x_ref, gain_ref, out_ref):
    for i, piece in scaled_heads(x_ref, gain_ref):
        out_ref[:, i * HD : (i + 1) * HD] = piece


def pair_kernel(k_ref, v_ref, gain_ref, out_ref):
    chans = k_ref.shape[1]
    for i, piece in scaled_heads(k_ref, gain_ref):
        out_ref[:, i * HD : (i + 1) * HD] = piece
    out_ref[:, chans:] = v_ref[...]


def norm(x, gain):
    return pl.pallas_call(
        norm_kernel,
        out_shape=jax.ShapeDtypeStruct(x.shape, jnp.bfloat16),
        in_specs=whole(2),
        out_specs=pl.BlockSpec(memory_space=pltpu.VMEM),
        compiler_params=LIMIT,
    )(x, gain.reshape(-1, HD))


def pair(keys, values, gain):
    rows, chans = keys.shape
    return pl.pallas_call(
        pair_kernel,
        out_shape=jax.ShapeDtypeStruct((rows, 2 * chans), jnp.bfloat16),
        in_specs=whole(3),
        out_specs=pl.BlockSpec(memory_space=pltpu.VMEM),
        compiler_params=LIMIT,
    )(keys, values, gain.reshape(-1, HD))


def attend_kernel(reach_ref, q_ref, kb_ref, k_ref, ka_ref, kd_ref, vb_ref, v_ref, va_ref, vd_ref, o_ref):
    scale = HD ** (-0.5)
    place = lax.axis_index("tm")
    peers = lax.axis_size("tm")
    seen = ((reach_ref[0, 0] == 1) & (place > 0), (reach_ref[0, 1] == 1) & (place < peers - 1))
    bias = [jnp.where(flag, 0.0, -1e30).astype(jnp.float32) for flag in seen]
    low = place % 4

    def three(before_ref, own_ref, after_ref, other_ref, at):
        other = other_ref[:, at]
        before = jnp.where(low == 0, other, before_ref[:, at])
        return before, own_ref[:, at], jnp.where(low == 3, other, after_ref[:, at])

    for h in range(q_ref.shape[1] // HD):
        at = slice(h * HD, (h + 1) * HD)
        query = q_ref[:, at]
        parts = []
        for key, extra in zip(three(kb_ref, k_ref, ka_ref, kd_ref, at), (bias[0], None, bias[1])):
            part = lax.dot_general(query, key, (((1,), (1,)), ((), ())), preferred_element_type=jnp.float32)
            part = part * scale
            parts.append(part if extra is None else part + extra)
        top = functools.reduce(jnp.maximum, [jnp.max(part, axis=-1, keepdims=True) for part in parts])
        expo = [jnp.exp(part - top) for part in parts]
        total = functools.reduce(jnp.add, [jnp.sum(part, axis=-1, keepdims=True) for part in expo])
        share = 1.0 / total
        out = None
        for part, value in zip(expo, three(vb_ref, v_ref, va_ref, vd_ref, at)):
            weights = (part * share).astype(jnp.bfloat16)
            term = jnp.dot(weights, value, preferred_element_type=jnp.float32)
            out = term if out is None else out + term
        o_ref[:, at] = out.astype(jnp.bfloat16)


def attend(reach, qn, pairs, chunk, chunks):
    rows, chans = qn.shape
    wide = chans // chunks
    heads = wide // HD
    step = next(n for n in (5, 4, 3, 2, 1) if heads % n == 0)
    cols = step * HD
    steps = wide // cols
    k_spec = pl.BlockSpec((rows, cols), lambda i: (0, chunk * steps + i))
    v_spec = pl.BlockSpec((rows, cols), lambda i: (0, (chunks + chunk) * steps + i))
    return pl.pallas_call(
        attend_kernel,
        grid=(steps,),
        out_shape=jax.ShapeDtypeStruct((rows, wide), jnp.bfloat16),
        in_specs=[pl.BlockSpec(memory_space=pltpu.SMEM)] + [k_spec] * 5 + [v_spec] * 4,
        out_specs=pl.BlockSpec((rows, cols), lambda i: (0, i)),
        compiler_params=LIMIT,
    )(reach, qn, *pairs, *pairs)


def project_kernel(share, count, slots, total, final, resumed, gate_ref, *refs):
    refs = list(refs)
    a_ref = refs.pop()
    base_ref = refs.pop(0) if resumed else None
    att_refs, w_refs = refs[:count], refs[count : count + len(slots)]
    outs = refs[count + len(slots) :]
    rows, wide = att_refs[0].shape
    depth, cols = w_refs[0].shape
    chunks = count // 2
    place = lax.axis_index("tm")
    line = place // 4
    for i, ref in enumerate(att_refs):
        p, j = i // chunks, i % chunks
        a_ref[p * rows : (p + 1) * rows, j * wide : (j + 1) * wide] = ref[...]
    acc = base_ref[...] if resumed else None
    for i, ref in zip(slots, w_refs):
        start = pl.multiple_of((line ^ i) * depth, HD) if total > 1 else 0
        term = jnp.dot(a_ref[:, pl.ds(start, depth)], ref[...], preferred_element_type=jnp.float32)
        acc = term if acc is None else acc + term
    if not final:
        outs[0][...] = acc
        return
    first = ((place % 4) * 2 + (lax.axis_index("groups") ^ share)) * (cols // HD)
    for p in range(2):
        for b in range(cols // HD):
            at = slice(b * HD, (b + 1) * HD)
            scaled = gate_ref[pl.ds(first + b, 1), :] * acc[p * rows : (p + 1) * rows, at]
            outs[p][:, at] = scaled.astype(jnp.bfloat16)


def project(gate, att, weights, share, slots, final=True, base=None):
    rows, wide = att[0].shape
    cols = weights[0].shape[1]
    used = [weights[i] for i in slots]
    resumed = [] if base is None else [base]
    if final:
        out = [jax.ShapeDtypeStruct((rows, cols), jnp.bfloat16)] * 2
    else:
        out = [jax.ShapeDtypeStruct((2 * rows, cols), jnp.float32)]
    body = functools.partial(project_kernel, share, len(att), slots, len(weights), final, bool(resumed))
    return pl.pallas_call(
        body,
        out_shape=out,
        in_specs=whole(1 + len(resumed) + len(att) + len(used)),
        out_specs=whole(len(out)),
        scratch_shapes=[pltpu.VMEM((2 * rows, wide * len(att) // 2), jnp.bfloat16)],
        compiler_params=LIMIT,
    )(gate.reshape(-1, HD), *resumed, *att, *used)


def place_kernel(spots, aliased, *refs):
    pieces, out_ref, sems = refs[aliased:-2], refs[-2], refs[-1]
    cols = pieces[0].shape[1]
    low = lax.axis_index("tm") % 4
    group = lax.axis_index("groups")
    copies = []
    for i, (ref, (near, share)) in enumerate(zip(pieces, spots)):
        start = pl.multiple_of(((low ^ near) * 2 + (group ^ share)) * cols, HD)
        copies.append(pltpu.make_async_copy(ref, out_ref.at[:, pl.ds(start, cols)], sems.at[i]))
    for copy in copies:
        copy.start()
    for copy in copies:
        copy.wait()


def place_pieces(base, pieces, spots):
    rows, cols = pieces[0].shape
    anywhere = pl.BlockSpec(memory_space=pl.ANY)
    aliased = 0 if base is None else 1
    return pl.pallas_call(
        functools.partial(place_kernel, spots, aliased),
        out_shape=jax.ShapeDtypeStruct((rows, cols * 8), jnp.bfloat16),
        in_specs=[anywhere] * aliased + whole(len(pieces)),
        out_specs=anywhere,
        scratch_shapes=[pltpu.SemaphoreType.DMA((len(pieces),))],
        input_output_aliases={0: 0} if aliased else {},
        compiler_params=LIMIT,
    )(*([] if base is None else [base]), *pieces)


def local(queries, keys, values, q_gain, k_gain, out_weight, out_gate, reach):
    peers = lax.axis_size("tm")
    place = lax.axis_index("tm")
    group = lax.axis_index("groups")
    low = place % 4
    line = place // 4
    lines = peers // 4
    _, width = out_weight.shape
    _, chans = queries.shape
    cols = width // 8
    chunks = 2 if chans // HD % 2 == 0 else 1

    def swap(x, bits):
        return lax.ppermute(x, "tm", [(i, i ^ bits) for i in range(peers)])

    def group_swap(x):
        return lax.ppermute(x, "groups", [(0, 1), (1, 0)])

    def along(x, moves):
        return lax.ppermute(x, "tm", [(4 * a + i, 4 * b + i) for a, b in moves for i in range(4)])

    def send(x, pairs):
        return lax.ppermute(x, "tm", pairs)

    up = [(i, i + 1) for i in range(peers - 1)]
    down = [(j, i) for i, j in up]

    def inside(pairs):
        return [(i, j) for i, j in pairs if i // 4 == j // 4]

    def choose(flag, a, b):
        return jnp.where(flag, a, b)

    def column(quarter, share):
        return (quarter * 2 + share) * cols

    def weight_part(quarter):
        return lax.dynamic_slice_in_dim(out_weight, column(quarter, group), cols, 1)

    cuts = lax.optimization_barrier([weight_part(low ^ i) for i in range(4)])
    parts = [cuts[0]] + [swap(cuts[i], i) for i in (1, 2, 3)]
    odd, upper = (low % 2) == 1, low >= 2
    halves = [
        jnp.concatenate([choose(odd, b, a), choose(odd, a, b)], axis=0)
        for a, b in ((parts[0], parts[1]), (parts[2], parts[3]))
    ]
    block = jnp.concatenate([choose(upper, halves[1], halves[0]), choose(upper, halves[0], halves[1])], axis=0)

    leap = [(4 * z + 3, 4 * z + 7) for z in range(lines - 1)] + [(4 * z + 4, 4 * z) for z in range(lines - 1)]
    turn = [(4 * z + i, 4 * z + (i ^ 3)) for z in range(lines) for i in (0, 3)]
    k_leap, v_leap = send(keys, leap), send(values, leap)
    kv = pair(keys, values, k_gain)
    near = [send(kv, inside(up)), kv, send(kv, inside(down))]
    near.append(send(pair(k_leap, v_leap, k_gain), turn))
    qn = norm(queries, q_gain)

    if lines == 4:
        middle = (line == 1) | (line == 2)
        beside = along(block, ((0, 1), (1, 0), (2, 3), (3, 2)))
        across = along(block, ((1, 2), (2, 1)))
        across_far = along(beside, ((1, 2), (2, 1)))
        edge = along(across, ((1, 0), (2, 3)))
        edge_far = along(across_far, ((1, 0), (2, 3)))
        second = choose(middle, across_far, edge)
        third = choose(middle, across, edge_far)
        slots = [block, beside, second, third]
    else:
        members = [[z * 4 + i for z in range(lines)] for i in range(4)]
        slots = [lax.all_gather(block, "tm", axis_index_groups=members, axis=0, tiled=True)]
    shares = [slots, [group_swap(slot) for slot in slots]]

    here, there = [], []
    for i in range(chunks):
        own = attend(reach, qn, near, i, chunks)
        over = swap(own, 2)
        here.append([own, swap(own, 1)])
        there.append([over, swap(over, 1)])
    here = [pair[p] for p in range(2) for pair in here]
    there = [pair[p] for p in range(2) for pair in there]
    pieces = {}
    every = tuple(range(len(slots)))
    for j in range(2):
        made = project(out_gate, here, shares[j], j, every)
        pieces[0, j], pieces[1, j] = made[0], swap(made[1], 1)
        base, rest = None, every
        if j == 1 and len(every) > 1:
            base = project(out_gate, there, shares[j], j, every[:-1], final=False)[0]
            rest = every[-1:]
        made = project(out_gate, there, shares[j], j, rest, base=base)
        pieces[2, j], pieces[3, j] = swap(made[0], 2), swap(made[1], 3)
    last = [(2, 1), (3, 1)]
    most = [spot for spot in pieces if spot not in last]
    out = place_pieces(None, [pieces[spot] for spot in most], most)
    return place_pieces(out, [pieces[spot] for spot in last], last)


def solution(mesh):
    return jax.shard_map(
        local,
        mesh=mesh,
        in_specs=(
            P(("groups", "tm"), None),
            P(("groups", "tm"), None),
            P(("groups", "tm"), None),
            P(),
            P(),
            P("tm", None),
            P(),
            P(("groups", "tm"), None),
        ),
        out_specs=P(("groups", "tm"), None),
        check_vma=False,
    )
```

```python
import functools

import jax
import jax.numpy as jnp
from jax import lax
from jax.experimental import pallas as pl
from jax.experimental.pallas import tpu as pltpu
from jax.sharding import PartitionSpec as P


HD = 128


LIMIT = pltpu.CompilerParams(vmem_limit_bytes=16 * 1024 * 1024)


def whole(count):
    return [pl.BlockSpec(memory_space=pltpu.VMEM)] * count


def scaled_heads(x_ref, gain_ref):
    block = x_ref[...].astype(jnp.float32)
    inverse = lax.rsqrt(jnp.mean(block * block, axis=-1, keepdims=True) + 1e-06)
    for i in range(x_ref.shape[1] // HD):
        piece = x_ref[:, i * HD : (i + 1) * HD].astype(jnp.float32)
        yield i, (piece * inverse * gain_ref[i : i + 1, :]).astype(jnp.bfloat16)


def norm_kernel(x_ref, gain_ref, out_ref):
    for i, piece in scaled_heads(x_ref, gain_ref):
        out_ref[:, i * HD : (i + 1) * HD] = piece


def pair_kernel(k_ref, v_ref, gain_ref, out_ref, kn_ref):
    chans = k_ref.shape[1]
    for i, piece in scaled_heads(k_ref, gain_ref):
        out_ref[:, i * HD : (i + 1) * HD] = piece
        kn_ref[:, i * HD : (i + 1) * HD] = piece
    out_ref[:, chans:] = v_ref[...]


def norm(x, gain):
    return pl.pallas_call(
        norm_kernel,
        out_shape=jax.ShapeDtypeStruct(x.shape, jnp.bfloat16),
        in_specs=whole(2),
        out_specs=pl.BlockSpec(memory_space=pltpu.VMEM),
        compiler_params=LIMIT,
    )(x, gain.reshape(-1, HD))


def pair(keys, values, gain):
    rows, chans = keys.shape
    return pl.pallas_call(
        pair_kernel,
        out_shape=[jax.ShapeDtypeStruct((rows, n * chans), jnp.bfloat16) for n in (2, 1)],
        in_specs=whole(3),
        out_specs=whole(2),
        compiler_params=LIMIT,
    )(keys, values, gain.reshape(-1, HD))


def attend_kernel(reach_ref, q_ref, kb_ref, k_ref, ka_ref, vb_ref, v_ref, va_ref, kd_ref, vd_ref, o_ref):
    scale = HD ** (-0.5)
    place = lax.axis_index("tm")
    peers = lax.axis_size("tm")
    seen = ((reach_ref[0, 0] == 1) & (place > 0), (reach_ref[0, 1] == 1) & (place < peers - 1))
    bias = [jnp.where(flag, 0.0, -1e30).astype(jnp.float32) for flag in seen]
    low = place % 4

    def three(before_ref, own_ref, after_ref, other_ref, at):
        other = other_ref[:, at]
        before = jnp.where(low == 0, other, before_ref[:, at])
        return before, own_ref[:, at], jnp.where(low == 3, other, after_ref[:, at])

    for h in range(q_ref.shape[1] // HD):
        at = slice(h * HD, (h + 1) * HD)
        query = q_ref[:, at]
        parts = []
        for key, extra in zip(three(kb_ref, k_ref, ka_ref, kd_ref, at), (bias[0], None, bias[1])):
            part = lax.dot_general(query, key, (((1,), (1,)), ((), ())), preferred_element_type=jnp.float32)
            part = part * scale
            parts.append(part if extra is None else part + extra)
        top = functools.reduce(jnp.maximum, [jnp.max(part, axis=-1, keepdims=True) for part in parts])
        expo = [jnp.exp(part - top) for part in parts]
        total = functools.reduce(jnp.add, [jnp.sum(part, axis=-1, keepdims=True) for part in expo])
        share = 1.0 / total
        out = None
        for part, value in zip(expo, three(vb_ref, v_ref, va_ref, vd_ref, at)):
            weights = (part * share).astype(jnp.bfloat16)
            term = jnp.dot(weights, value, preferred_element_type=jnp.float32)
            out = term if out is None else out + term
        o_ref[:, at] = out.astype(jnp.bfloat16)


def attend(reach, qn, pairs, k_diag, v_diag, chunk, chunks):
    rows, chans = qn.shape
    wide = chans // chunks
    heads = wide // HD
    step = next(n for n in (5, 4, 3, 2, 1) if heads % n == 0)
    cols = step * HD
    steps = wide // cols
    k_spec = pl.BlockSpec((rows, cols), lambda i: (0, chunk * steps + i))
    v_spec = pl.BlockSpec((rows, cols), lambda i: (0, (chunks + chunk) * steps + i))
    return pl.pallas_call(
        attend_kernel,
        grid=(steps,),
        out_shape=jax.ShapeDtypeStruct((rows, wide), jnp.bfloat16),
        in_specs=[pl.BlockSpec(memory_space=pltpu.SMEM)] + [k_spec] * 4 + [v_spec] * 3 + [k_spec] * 2,
        out_specs=pl.BlockSpec((rows, cols), lambda i: (0, i)),
        compiler_params=LIMIT,
    )(reach, qn, *pairs, *pairs, k_diag, v_diag)


def join_kernel(*refs):
    pieces, out_ref = refs[:-1], refs[-1]
    depth = pieces[0].shape[0]
    low = lax.axis_index("tm") % 4
    for i, ref in enumerate(pieces):
        out_ref[pl.ds(pl.multiple_of((low ^ i) * depth, depth), depth), :] = ref[...]


def join(pieces):
    depth, cols = pieces[0].shape
    return pl.pallas_call(
        join_kernel,
        out_shape=jax.ShapeDtypeStruct((4 * depth, cols), jnp.bfloat16),
        in_specs=whole(4),
        out_specs=pl.BlockSpec(memory_space=pltpu.VMEM),
        compiler_params=LIMIT,
        name="join",
    )(*pieces)


def pick_kernel(inner_ref, outer_ref, out_ref):
    line = lax.axis_index("tm") // 4
    inner = (line > 0) & (line < lax.axis_size("tm") // 4 - 1)

    @pl.when(inner)
    def _():
        out_ref[...] = inner_ref[...]

    @pl.when(jnp.logical_not(inner))
    def _():
        out_ref[...] = outer_ref[...]


def pick(inner, outer):
    return pl.pallas_call(
        pick_kernel,
        out_shape=jax.ShapeDtypeStruct(inner.shape, inner.dtype),
        in_specs=whole(2),
        out_specs=pl.BlockSpec(memory_space=pltpu.VMEM),
        compiler_params=LIMIT,
    )(inner, outer)


def project_kernel(share, count, slots, total, final, resumed, gate_ref, *refs):
    refs = list(refs)
    a_ref = refs.pop()
    base_ref = refs.pop(0) if resumed else None
    att_refs, w_refs = refs[:count], refs[count : count + len(slots)]
    outs = refs[count + len(slots) :]
    rows, wide = att_refs[0].shape
    depth, cols = w_refs[0].shape
    chunks = count // 2
    place = lax.axis_index("tm")
    line = place // 4
    for i, ref in enumerate(att_refs):
        p, j = i // chunks, i % chunks
        a_ref[p * rows : (p + 1) * rows, j * wide : (j + 1) * wide] = ref[...]
    acc = base_ref[...] if resumed else None
    for i, ref in zip(slots, w_refs):
        start = pl.multiple_of((line ^ i) * depth, HD) if total > 1 else 0
        term = jnp.dot(a_ref[:, pl.ds(start, depth)], ref[...], preferred_element_type=jnp.float32)
        acc = term if acc is None else acc + term
    if not final:
        outs[0][...] = acc
        return
    first = ((place % 4) * 2 + (lax.axis_index("groups") ^ share)) * (cols // HD)
    for p in range(2):
        for b in range(cols // HD):
            at = slice(b * HD, (b + 1) * HD)
            scaled = gate_ref[pl.ds(first + b, 1), :] * acc[p * rows : (p + 1) * rows, at]
            outs[p][:, at] = scaled.astype(jnp.bfloat16)


def project(gate, att, weights, share, slots, final=True, base=None):
    rows, wide = att[0].shape
    cols = weights[0].shape[1]
    used = [weights[i] for i in slots]
    resumed = [] if base is None else [base]
    if final:
        out = [jax.ShapeDtypeStruct((rows, cols), jnp.bfloat16)] * 2
    else:
        out = [jax.ShapeDtypeStruct((2 * rows, cols), jnp.float32)]
    body = functools.partial(project_kernel, share, len(att), slots, len(weights), final, bool(resumed))
    return pl.pallas_call(
        body,
        out_shape=out,
        in_specs=whole(1 + len(resumed) + len(att) + len(used)),
        out_specs=whole(len(out)),
        scratch_shapes=[pltpu.VMEM((2 * rows, wide * len(att) // 2), jnp.bfloat16)],
        compiler_params=LIMIT,
    )(gate.reshape(-1, HD), *resumed, *att, *used)


def place_kernel(spots, aliased, *refs):
    pieces, out_ref, sems = refs[aliased:-2], refs[-2], refs[-1]
    cols = pieces[0].shape[1]
    low = lax.axis_index("tm") % 4
    group = lax.axis_index("groups")
    copies = []
    for i, (ref, (near, share)) in enumerate(zip(pieces, spots)):
        start = pl.multiple_of(((low ^ near) * 2 + (group ^ share)) * cols, HD)
        copies.append(pltpu.make_async_copy(ref, out_ref.at[:, pl.ds(start, cols)], sems.at[i]))
    for copy in copies:
        copy.start()
    for copy in copies:
        copy.wait()


def place_pieces(base, pieces, spots):
    rows, cols = pieces[0].shape
    anywhere = pl.BlockSpec(memory_space=pl.ANY)
    aliased = 0 if base is None else 1
    return pl.pallas_call(
        functools.partial(place_kernel, spots, aliased),
        out_shape=jax.ShapeDtypeStruct((rows, cols * 8), jnp.bfloat16),
        in_specs=[anywhere] * aliased + whole(len(pieces)),
        out_specs=anywhere,
        scratch_shapes=[pltpu.SemaphoreType.DMA((len(pieces),))],
        input_output_aliases={0: 0} if aliased else {},
        compiler_params=LIMIT,
    )(*([] if base is None else [base]), *pieces)


def local(queries, keys, values, q_gain, k_gain, out_weight, out_gate, reach):
    peers = lax.axis_size("tm")
    place = lax.axis_index("tm")
    group = lax.axis_index("groups")
    low = place % 4
    lines = peers // 4
    depth, width = out_weight.shape
    _, chans = queries.shape
    cols = width // 8
    chunks = 2 if chans // HD % 2 == 0 else 1

    def swap(x, bits):
        return lax.ppermute(x, "tm", [(i, i ^ bits) for i in range(peers)])

    def group_swap(x):
        return lax.ppermute(x, "groups", [(0, 1), (1, 0)])

    def along(x, moves):
        return lax.ppermute(x, "tm", [(4 * a + i, 4 * b + i) for a, b in moves for i in range(4)])

    def send(x, pairs):
        return lax.ppermute(x, "tm", pairs)

    up = [(i, i + 1) for i in range(peers - 1)]
    down = [(j, i) for i, j in up]

    def inside(pairs):
        return [(i, j) for i, j in pairs if i // 4 == j // 4]

    def outside(pairs):
        return [(i, j) for i, j in pairs if i // 4 != j // 4]

    def choose(flag, a, b):
        return jnp.where(flag, a, b)

    def column(quarter, share):
        return (quarter * 2 + share) * cols

    def weight_part(quarter):
        return lax.dynamic_slice_in_dim(out_weight, column(quarter, group), cols, 1)

    cuts = lax.optimization_barrier([weight_part(low ^ i) for i in range(4)])
    parts = [cuts[0]] + [swap(cuts[i], i) for i in (1, 2, 3)]
    if depth % 16 == 0:
        block = join(parts)
    else:
        odd, upper = (low % 2) == 1, low >= 2
        halves = [
            jnp.concatenate([choose(odd, b, a), choose(odd, a, b)], axis=0)
            for a, b in ((parts[0], parts[1]), (parts[2], parts[3]))
        ]
        block = jnp.concatenate([choose(upper, halves[1], halves[0]), choose(upper, halves[0], halves[1])], axis=0)

    kv, kn = pair(keys, values, k_gain)
    near = [send(kv, inside(up)), kv, send(kv, inside(down))]
    k_diag = send(kn, outside(up) + outside(down))
    turn = [(4 * z + i, 4 * z + (i ^ 2)) for z in range(lines) for i in (0, 3)]
    leap = [(i ^ 2, j) for i, j in outside(up) + outside(down)]
    v_diag = send(send(values, turn), leap)
    qn = norm(queries, q_gain)

    if lines == 4:
        beside = along(block, ((0, 1), (1, 0), (2, 3), (3, 2)))
        across = along(block, ((1, 2), (2, 1)))
        across_far = along(beside, ((1, 2), (2, 1)))
        edge = along(across, ((1, 0), (2, 3)))
        edge_far = along(across_far, ((1, 0), (2, 3)))
        second = pick(across_far, edge)
        third = pick(across, edge_far)
        slots = [block, beside, second, third]
    else:
        members = [[z * 4 + i for z in range(lines)] for i in range(4)]
        slots = [lax.all_gather(block, "tm", axis_index_groups=members, axis=0, tiled=True)]
    shares = [slots, [group_swap(slot) for slot in slots]]

    here, there = [], []
    for i in range(chunks):
        own = attend(reach, qn, near, k_diag, v_diag, i, chunks)
        over = swap(own, 2)
        here.append([own, swap(own, 1)])
        there.append([over, swap(over, 1)])
    here = [pair[p] for p in range(2) for pair in here]
    there = [pair[p] for p in range(2) for pair in there]
    pieces = {}
    every = tuple(range(len(slots)))
    for j in range(2):
        made = project(out_gate, here, shares[j], j, every)
        pieces[0, j], pieces[1, j] = made[0], swap(made[1], 1)
        base, rest = None, every
        if j == 1 and len(every) > 1:
            base = project(out_gate, there, shares[j], j, every[:-1], final=False)[0]
            rest = every[-1:]
        made = project(out_gate, there, shares[j], j, rest, base=base)
        pieces[2, j], pieces[3, j] = swap(made[0], 2), swap(made[1], 3)
    last = [(2, 1), (3, 1)]
    most = [spot for spot in pieces if spot not in last]
    out = place_pieces(None, [pieces[spot] for spot in most], most)
    return place_pieces(out, [pieces[spot] for spot in last], last)


def solution(mesh):
    return jax.shard_map(
        local,
        mesh=mesh,
        in_specs=(
            P(("groups", "tm"), None),
            P(("groups", "tm"), None),
            P(("groups", "tm"), None),
            P(),
            P(),
            P("tm", None),
            P(),
            P(("groups", "tm"), None),
        ),
        out_specs=P(("groups", "tm"), None),
        check_vma=False,
    )
```
